8 devices in a mesh: dp: 1 (over z), tp: 2 (over y), ep: 4 (over x, core).
Axes of the slice: x: 2, y: 2, z: 1, core: 2. Of those that a mesh axis runs over, the one named last changes fastest.
Arguments:
- normed: bfloat16 [512, 1280], P(('dp', 'ep'))
- residual: bfloat16 [512, 1280], P(('dp', 'ep'))
- w_router: float32 [1280, 64], replicated
- ws_gate: bfloat16 [1280, 1792], P(None, 'tp')
- ws_up: bfloat16 [1280, 1792], P(None, 'tp')
- ws_down: bfloat16 [1792, 1280], P('tp')
- we_gate: bfloat16 [64, 1280, 896], P('ep', None, 'tp')
- we_up: bfloat16 [64, 1280, 896], P('ep', None, 'tp')
- we_down: bfloat16 [64, 896, 1280], P('ep', 'tp')
- first_id: int32 [512], P(('dp', 'ep'))
- alt_id: int32 [512], P(('dp', 'ep'))
Outputs:
- output: bfloat16 [512, 1280], P(('dp', 'ep'))
All inputs are finite; a program needn't handle non-finite values.
Results may differ from the reference program's by a relative error of at most 0.00502053.
Values are sent between devices in bfloat16 or wider.
A program may use at most 1 GiB of HBM per device.

```python
import jax
import jax.numpy as jnp
from jax import lax

TOK_DEV = 128
EP_RANKS = 4
EXPERTS = 64
D_MODEL = 1280
FF_EXPERT = 896
FF_SHARED = 1792
HOT_COUNT = 4
HOT_WEIGHT = 3

TOKENS = TOK_DEV * EP_RANKS
LOCAL_EXPERTS = EXPERTS // EP_RANKS
CAPACITY = (5 * TOKENS + 4 * EXPERTS - 1) // (4 * EXPERTS)


def draw_routing(route_key):
    key_list = jax.random.split(route_key, 6)
    hot_flag = (jax.random.permutation(key_list[0], EXPERTS) < HOT_COUNT).astype(jnp.int32)
    cum_weight = jnp.cumsum((1 + (HOT_WEIGHT - 1) * hot_flag).reshape(EP_RANKS, LOCAL_EXPERTS), axis=1)
    owner_quota = jnp.arange(TOK_DEV, dtype=jnp.int32) % EP_RANKS
    owner_first = jax.vmap(lambda key_one: jax.random.permutation(key_one, owner_quota))(jax.random.split(key_list[1], EP_RANKS))
    owner_alt = jax.vmap(lambda key_one: jax.random.permutation(key_one, owner_quota))(jax.random.split(key_list[2], EP_RANKS))
    row_cum = cum_weight[owner_first]
    draw_value = jax.random.randint(key_list[3], (EP_RANKS, TOK_DEV), 0, row_cum[:, :, -1])
    local_first = jnp.sum((row_cum <= draw_value[:, :, None]).astype(jnp.int32), axis=2)
    alt_shift = jax.random.randint(key_list[4], (EP_RANKS, TOK_DEV), 1, LOCAL_EXPERTS)
    free_pick = jax.random.randint(key_list[5], (EP_RANKS, TOK_DEV), 0, LOCAL_EXPERTS)
    local_alt = jnp.where(owner_alt == owner_first, (local_first + alt_shift) % LOCAL_EXPERTS, free_pick)
    first_id = (owner_first * LOCAL_EXPERTS + local_first).reshape(TOKENS).astype(jnp.int32)
    alt_id = (owner_alt * LOCAL_EXPERTS + local_alt).reshape(TOKENS).astype(jnp.int32)
    return first_id, alt_id


def setup_inputs(seed: int = 0, part: int = 0) -> dict:
    root_key = jax.random.key(seed)
    part_keys = jax.random.split(jax.random.fold_in(root_key, part), 3)
    weight_keys = jax.random.split(root_key, 7)
    normed = jax.random.normal(part_keys[0], (TOKENS, D_MODEL), jnp.float32).astype(jnp.bfloat16)
    residual = jax.random.normal(part_keys[1], (TOKENS, D_MODEL), jnp.float32).astype(jnp.bfloat16)
    first_id, alt_id = draw_routing(part_keys[2])
    w_router = jax.random.normal(weight_keys[0], (D_MODEL, EXPERTS), jnp.float32) * D_MODEL ** -0.5
    ws_gate = (jax.random.normal(weight_keys[1], (D_MODEL, FF_SHARED), jnp.float32) * D_MODEL ** -0.5).astype(jnp.bfloat16)
    ws_up = (jax.random.normal(weight_keys[2], (D_MODEL, FF_SHARED), jnp.float32) * D_MODEL ** -0.5).astype(jnp.bfloat16)
    ws_down = (jax.random.normal(weight_keys[3], (FF_SHARED, D_MODEL), jnp.float32) * FF_SHARED ** -0.5).astype(jnp.bfloat16)
    we_gate = (jax.random.normal(weight_keys[4], (EXPERTS, D_MODEL, FF_EXPERT), jnp.float32) * D_MODEL ** -0.5).astype(jnp.bfloat16)
    we_up = (jax.random.normal(weight_keys[5], (EXPERTS, D_MODEL, FF_EXPERT), jnp.float32) * D_MODEL ** -0.5).astype(jnp.bfloat16)
    we_down = (jax.random.normal(weight_keys[6], (EXPERTS, FF_EXPERT, D_MODEL), jnp.float32) * (EXPERTS * FF_EXPERT ** -0.5)).astype(jnp.bfloat16)
    return {'normed': normed, 'residual': residual, 'w_router': w_router, 'ws_gate': ws_gate, 'ws_up': ws_up, 'ws_down': ws_down, 'we_gate': we_gate, 'we_up': we_up, 'we_down': we_down, 'first_id': first_id, 'alt_id': alt_id}


def expert_mlp(token_rows, w_gate, w_up, w_down):
    gate_pre = jnp.dot(token_rows, w_gate, preferred_element_type=jnp.float32)
    up_pre = jnp.dot(token_rows, w_up, preferred_element_type=jnp.float32)
    hidden_act = (jax.nn.silu(gate_pre) * up_pre).astype(jnp.bfloat16)
    return jnp.dot(hidden_act, w_down, preferred_element_type=jnp.float32)


def rank_in_column(onehot):
    return jnp.sum(jnp.cumsum(onehot, axis=0) * onehot, axis=1) - 1


def reference(normed, residual, w_router, ws_gate, ws_up, ws_down, we_gate, we_up, we_down, first_id, alt_id):
    expert_ids = jnp.arange(EXPERTS, dtype=jnp.int32)
    onehot_first = (first_id[:, None] == expert_ids[None, :]).astype(jnp.int32)
    rank_first = rank_in_column(onehot_first)
    kept_mask = rank_first < CAPACITY
    slot_load = jnp.minimum(jnp.sum(onehot_first, axis=0), CAPACITY)
    overflow = jnp.logical_not(kept_mask)
    onehot_alt = ((alt_id[:, None] == expert_ids[None, :]) & overflow[:, None]).astype(jnp.int32)
    rank_alt = rank_in_column(onehot_alt)
    recycled = overflow & (rank_alt < (CAPACITY - slot_load)[alt_id])
    active = kept_mask | recycled
    chosen = jnp.where(kept_mask, first_id, alt_id)
    slot_index = jnp.where(kept_mask, rank_first, slot_load[alt_id] + rank_alt)
    table_size = EXPERTS * CAPACITY
    slot_code = jnp.where(active, chosen * CAPACITY + slot_index, table_size)
    slot_token = jnp.full((table_size,), TOKENS, jnp.int32).at[slot_code].set(jnp.arange(TOKENS, dtype=jnp.int32), mode='drop')
    slot_rows = jnp.take(normed, slot_token, axis=0, mode='fill', fill_value=0).reshape(EXPERTS, CAPACITY, D_MODEL)
    routed_slots = lax.map(lambda bundle: expert_mlp(bundle[0], bundle[1], bundle[2], bundle[3]).astype(jnp.bfloat16), (slot_rows, we_gate, we_up, we_down))
    routed = jnp.take(routed_slots.reshape(table_size, D_MODEL), jnp.minimum(slot_code, table_size - 1), axis=0)
    router_prob = jax.nn.softmax(jnp.dot(normed, w_router, preferred_element_type=jnp.float32), axis=-1)
    gate_weight = jnp.take_along_axis(router_prob, chosen[:, None], axis=1)[:, 0] * active.astype(jnp.float32)
    shared = lax.map(lambda block_rows: expert_mlp(block_rows, ws_gate, ws_up, ws_down), normed.reshape(EP_RANKS, TOK_DEV, D_MODEL)).reshape(TOKENS, D_MODEL)
    combined = residual.astype(jnp.float32) + shared + gate_weight[:, None] * routed.astype(jnp.float32)
    return combined.astype(jnp.bfloat16)
```

```python
import functools

import jax
import jax.numpy as jnp
from jax import lax
from jax.experimental import pallas as pl
from jax.experimental.pallas import tpu as pltpu
from jax.sharding import PartitionSpec as P

MESH = pl.DeviceIdType.MESH
F32, BF16, I32 = jnp.float32, jnp.bfloat16, jnp.int32

EP = 4
TOK = 128
ALL = EP * TOK
EXPERTS = 64
LOCAL = EXPERTS // EP
CAP = 10
SLOT = 16
SLOTS = LOCAL * SLOT
PAIR = 64
D = 1280
FFE = 448
FFS = 896
GRP = 4
NGRP = LOCAL // GRP
KC = ((0, 512), (512, 512), (1024, 256))
NC = 256
NCH = D // NC


def nn(a, b):
    return lax.dot_general(a, b, (((1,), (0,)), ((), ())), preferred_element_type=F32)


def nt(a, b):
    return lax.dot_general(a, b, (((1,), (1,)), ((), ())), preferred_element_type=F32)


def silu_mul(g, u):
    return (g * (1.0 / (1.0 + jnp.exp(-g))) * u).astype(BF16)


def kernel(normed, residual, wr, wsg, wsu, wsd, weg, weu, wed, fid, aid, out_ref,
           x0, x1, x2, res_v, wr_v, fids, aids,
           sg, su, sd, w1g, w1u, w2g, w2u, w3g, w3u,
           xs0, xs1, xs2, accg, accu, hid, hid_s,
           sh_part, sh_recv, gmat, tmat, gcol, csend, crecv, ypart, yrecv, slot_out,
           x_sem, id_sem, misc_sem, sw_sem, w_sem, d_sem,
           xs_send, xs_recv, id_send, id_recv, sh_sem, c_send, c_recv, y_send, y_recv):
    me = lax.axis_index("ep")
    tp = lax.axis_index("tp")
    xpeer = lax.rem(me + 2, EP)
    cpeer = me + 1 - 2 * lax.rem(me, 2)
    diag = lax.rem(cpeer + 2, EP)
    xr = (x0, x1, x2)
    xsr = (xs0, xs1, xs2)
    wgr, wur = (w1g, w2g, w3g), (w1u, w2u, w3u)
    mine = pl.ds(pl.multiple_of(me * TOK, TOK), TOK)

    def start(c):
        c.start()
        return c

    idc = [start(pltpu.make_async_copy(fid, fids.at[me], id_sem.at[0])),
           start(pltpu.make_async_copy(aid, aids.at[me], id_sem.at[1]))]
    xc = [start(pltpu.make_async_copy(normed.at[:, pl.ds(k, n)], xr[c].at[mine], x_sem.at[c])) for c, (k, n) in enumerate(KC)]
    wrc = start(pltpu.make_async_copy(wr, wr_v, misc_sem.at[0]))
    swc = [start(pltpu.make_async_copy(s, d, sw_sem.at[i])) for i, (s, d) in enumerate(((wsg, sg), (wsu, su), (wsd, sd)))]

    def gu_copy(p, g, i):
        k, n = KC[p]
        src = (weg, weu)[i].at[pl.ds(GRP * g, GRP), :, pl.ds(k, n)]
        return pltpu.make_async_copy(src, (wgr, wur)[i][p].at[pl.ds(GRP * g, GRP)], w_sem.at[p, g, i])

    def d_copy(j, g):
        ref, col = ((w1g, 0), (w1g, NC), (w1u, 0), (w1u, NC), (w2g, 0))[j]
        return pltpu.make_async_copy(wed.at[pl.ds(GRP * g, GRP), :, pl.ds(j * NC, NC)],
                                     ref.at[pl.ds(GRP * g, GRP), :, pl.ds(col, NC)], d_sem.at[j, g])

    def start_pass(p):
        for g in range(NGRP):
            for i in range(2):
                gu_copy(p, g, i).start()

    start_pass(0)
    resc = start(pltpu.make_async_copy(residual, res_v, misc_sem.at[1]))

    bar = pltpu.get_barrier_semaphore()
    for o in (xpeer, cpeer, diag):
        pl.semaphore_signal(bar, inc=1, device_id={"ep": o}, device_id_type=MESH)
    pl.semaphore_signal(bar, inc=1, device_id={"tp": 1 - tp}, device_id_type=MESH)
    pl.semaphore_wait(bar, 4)

    sends = []

    def rcopy(src, dst, s, r, **dev):
        c = pltpu.make_async_remote_copy(src_ref=src, dst_ref=dst, send_sem=s, recv_sem=r, device_id=dev, device_id_type=MESH)
        c.start()
        sends.append(c)
        return c

    for c in idc:
        c.wait()
    idr = []
    for d in range(1, EP):
        o = lax.rem(me + d, EP)
        for i, ref in enumerate((fids, aids)):
            idr.append(rcopy(ref.at[me], ref.at[me], id_send.at[i, d - 1], id_recv.at[i, d - 1], ep=o))
    xsend, csnd, fwd = [], [], []
    for c in range(3):
        xc[c].wait()
        xsend.append(rcopy(xr[c].at[mine], xr[c].at[mine], xs_send.at[0, c], xs_recv.at[0, c], ep=xpeer))
    for c in range(3):
        csnd.append(rcopy(xr[c].at[mine], xr[c].at[mine], xs_send.at[1, c], xs_recv.at[1, c], ep=cpeer))

    theirs = pl.ds(pl.multiple_of(xpeer * TOK, TOK), TOK)

    def forward(c):
        xsend[c].wait_recv()
        fwd.append(rcopy(xr[c].at[theirs], xr[c].at[theirs], xs_send.at[2, c], xs_recv.at[2, c], ep=cpeer))

    xo = [xr[c][mine, :] for c in range(3)]
    swc[0].wait()
    swc[1].wait()
    for n0 in range(0, FFS, 256):
        n = min(256, FFS - n0)
        g = sum(nn(xr[c][mine, :], sg[k:k + kn, n0:n0 + n]) for c, (k, kn) in enumerate(KC))
        u = sum(nn(xr[c][mine, :], su[k:k + kn, n0:n0 + n]) for c, (k, kn) in enumerate(KC))
        hid_s[:, n0:n0 + n] = silu_mul(g, u)
    swc[2].wait()
    for n0 in range(0, D, 256):
        sh_part[:, n0:n0 + 256] = nn(hid_s[...], sd[:, n0:n0 + 256]).astype(BF16)
    start_pass(1)
    start_pass(2)

    wrc.wait()
    wr_hi = wr_v[...].astype(BF16)
    wr_lo = (wr_v[...] - wr_hi.astype(F32)).astype(BF16)
    logits = jnp.zeros((TOK, EXPERTS), F32)
    for c, (k, kn) in enumerate(KC):
        logits = logits + nt(xo[c], wr_hi[:, k:k + kn]) + nt(xo[c], wr_lo[:, k:k + kn])
    ex = jnp.exp(logits - jnp.max(logits, axis=1, keepdims=True))
    prob = ex / jnp.sum(ex, axis=1, keepdims=True)
    shc = rcopy(sh_part, sh_recv, sh_sem.at[0], sh_sem.at[1], tp=1 - tp)

    for c in idr:
        c.wait_recv()
    f = jnp.concatenate([fids[o] for o in range(EP)], axis=1)
    a = jnp.concatenate([aids[o] for o in range(EP)], axis=1)
    ti, tj = lax.broadcasted_iota(I32, (ALL, ALL), 0), lax.broadcasted_iota(I32, (ALL, ALL), 1)
    before = jnp.where(ti < tj, 1.0, 0.0)
    before_dev = jnp.where((ti // TOK) == (tj // TOK), before, 0.0).astype(BF16)
    before = before.astype(BF16)
    eio = lax.broadcasted_iota(I32, (EXPERTS, ALL), 0)
    one_f = jnp.where(eio == f, 1.0, 0.0)
    one_a = jnp.where(eio == a, 1.0, 0.0)
    rank_f = jnp.sum(nn(one_f.astype(BF16), before) * one_f, axis=0, keepdims=True)
    kept = rank_f < CAP - 0.5
    load = jnp.minimum(jnp.sum(one_f, axis=1, keepdims=True), float(CAP))
    over_a = one_a * jnp.where(kept, 0.0, 1.0)
    rank_a = jnp.sum(nn(over_a.astype(BF16), before) * over_a, axis=0, keepdims=True)
    load_a = jnp.sum(one_a * load, axis=0, keepdims=True)
    active = kept | (rank_a + load_a < CAP - 0.5)
    chosen = jnp.where(kept, f, a)
    slot = jnp.where(kept, rank_f, load_a + rank_a).astype(I32)
    owner = chosen // LOCAL
    local = chosen - owner * LOCAL
    here = active & (owner == me)
    slot_code = jnp.where(here, local * SLOT + slot, -1)
    oio = lax.broadcasted_iota(I32, (16, ALL), 0)
    own_f = jnp.where(oio == f // LOCAL, 1.0, 0.0)
    own_a = jnp.where(oio == a // LOCAL + EP, 1.0, 0.0)
    seen = nn((own_f + own_a).astype(BF16), before_dev)
    pos_f = jnp.sum(seen * own_f, axis=0, keepdims=True)
    pos_a = jnp.sum(seen * own_a, axis=0, keepdims=True)
    pos = jnp.where(kept, pos_f, pos_a + PAIR // 2).astype(I32)
    origin = lax.broadcasted_iota(I32, (1, ALL), 1) // TOK
    pair_code = jnp.where(here, origin * PAIR + pos, -1)
    back_code = jnp.where(active, owner * PAIR + pos, -1)
    sio = lax.broadcasted_iota(I32, (SLOTS, ALL), 0)
    smat = jnp.where(sio == slot_code, 1.0, 0.0).astype(BF16)
    rmat = jnp.where(sio == pair_code, 1.0, 0.0).astype(BF16)
    gmat[...] = nt(rmat, smat).astype(BF16)

    own_back, own_chosen = back_code[:, :TOK], jnp.where(active, chosen, -1)[:, :TOK]
    all_chosen = jnp.where(active, chosen, -1)
    for o in range(1, EP):
        cols = slice(o * TOK, (o + 1) * TOK)
        own_back = jnp.where(me == o, back_code[:, cols], own_back)
        own_chosen = jnp.where(me == o, all_chosen[:, cols], own_chosen)
    eye = jnp.where(lax.broadcasted_iota(I32, (TOK, TOK), 0) == lax.broadcasted_iota(I32, (TOK, TOK), 1), 1.0, 0.0).astype(BF16)
    bio = lax.broadcasted_iota(I32, (EP * PAIR, TOK), 0)
    tmat[...] = nt(eye, jnp.where(bio == own_back, 1.0, 0.0).astype(BF16)).astype(BF16)
    cio = lax.broadcasted_iota(I32, (EXPERTS, TOK), 0)
    pick = nt(eye, jnp.where(cio == own_chosen, 1.0, 0.0).astype(BF16))
    gcol[...] = jnp.sum(prob * pick, axis=1, keepdims=True)

    def gather(c):
        csnd[c].wait_recv()
        fwd[c].wait_recv()
        xsr[c][...] = nn(smat, xr[c][...]).astype(BF16)

    def gu_pass(p, lo, hi):
        @pl.loop(lo, hi)
        def _(g):
            gu_copy(p, g, 0).wait()
            gu_copy(p, g, 1).wait()
            for i in range(GRP):
                e = g * GRP + i
                rows = pl.ds(pl.multiple_of(e * SLOT, SLOT), SLOT)
                xe = xsr[p][rows, :]
                dg, du = nt(xe, wgr[p][e]), nt(xe, wur[p][e])
                if p == 0:
                    accg[rows, :] = dg
                    accu[rows, :] = du
                elif p == 1:
                    accg[rows, :] += dg
                    accu[rows, :] += du
                else:
                    hid[rows, :] = silu_mul(accg[rows, :] + dg, accu[rows, :] + du)

    forward(0)
    gather(0)
    gu_pass(0, 0, NGRP)
    forward(1)
    for j in range(NCH - 1):
        for g in range(NGRP):
            d_copy(j, g).start()
    gather(1)
    gu_pass(1, 0, 2)
    forward(2)
    gu_pass(1, 2, NGRP)
    for g in range(NGRP):
        d_copy(NCH - 1, g).start()
    gather(2)
    gu_pass(2, 0, NGRP)

    cr = []
    my_rows = pl.ds(pl.multiple_of(me * PAIR, PAIR), PAIR)
    for j in range(NCH):
        ref, col = ((w1g, 0), (w1g, NC), (w1u, 0), (w1u, NC), (w2g, 0))[j]

        @pl.loop(0, NGRP)
        def _(g):
            d_copy(j, g).wait()
            for i in range(GRP):
                e = g * GRP + i
                rows = pl.ds(pl.multiple_of(e * SLOT, SLOT), SLOT)
                slot_out[rows, :] = nn(hid[rows, :], ref[e, :, col:col + NC]).astype(BF16)

        csend[j] = nn(gmat[...], slot_out[...]).astype(BF16)
        crecv[j, my_rows, :] = csend[j, my_rows, :]
        row = []
        for d in range(1, EP):
            o = lax.rem(me + d, EP)
            row.append(rcopy(csend.at[j, pl.ds(pl.multiple_of(o * PAIR, PAIR), PAIR)], crecv.at[j, my_rows],
                             c_send.at[j, d - 1], c_recv.at[j, d - 1], ep=o))
        cr.append(row)

    yr = []
    for j in range(NCH):
        for c in cr[j]:
            c.wait_recv()
        ypart[j] = nn(tmat[...], crecv[j]).astype(BF16)
        yr.append(rcopy(ypart.at[j], yrecv.at[j], y_send.at[j], y_recv.at[j], tp=1 - tp))

    resc.wait()
    shc.wait_recv()
    for j in range(NCH):
        cols = slice(j * NC, (j + 1) * NC)
        base = res_v[:, cols].astype(F32) + (sh_part[:, cols].astype(F32) + sh_recv[:, cols].astype(F32))
        yr[j].wait_recv()
        routed = (ypart[j].astype(F32) + yrecv[j].astype(F32)).astype(BF16).astype(F32)
        out_ref[:, cols] = (base + gcol[...] * routed).astype(BF16)
    for c in sends:
        c.wait_send()


def solution(mesh):
    tok_spec, id_spec = P(("dp", "ep"), None), P(("dp", "ep"))

    def device_step(normed, residual, w_router, ws_gate, ws_up, ws_down, we_gate, we_up, we_down, first_id, alt_id):
        hbm = pl.BlockSpec(memory_space=pl.ANY)
        vm, dma = pltpu.VMEM, pltpu.SemaphoreType.DMA
        weights = [vm((LOCAL, FFE, n), BF16) for _, n in KC for _ in range(2)]
        scratch = [vm((ALL, n), BF16) for _, n in KC]
        scratch += [vm((TOK, D), BF16), vm((EXPERTS, D), F32), vm((EP, 1, TOK), I32), vm((EP, 1, TOK), I32)]
        scratch += [vm((D, FFS), BF16), vm((D, FFS), BF16), vm((FFS, D), BF16)] + weights
        scratch += [vm((SLOTS, n), BF16) for _, n in KC]
        scratch += [vm((SLOTS, FFE), F32), vm((SLOTS, FFE), F32), vm((SLOTS, FFE), BF16), vm((TOK, FFS), BF16)]
        scratch += [vm((TOK, D), BF16), vm((TOK, D), BF16), vm((EP * PAIR, SLOTS), BF16), vm((TOK, EP * PAIR), BF16), vm((TOK, 1), F32)]
        scratch += [vm((NCH, EP * PAIR, NC), BF16), vm((NCH, EP * PAIR, NC), BF16), vm((NCH, TOK, NC), BF16), vm((NCH, TOK, NC), BF16), vm((SLOTS, NC), BF16)]
        scratch += [dma((3,)), dma((2,)), dma((2,)), dma((3,)), dma((3, NGRP, 2)), dma((NCH, NGRP)),
                    dma((3, 3)), dma((3, 3)), dma((2, 3)), dma((2, 3)), dma((2,)), dma((NCH, 3)), dma((NCH, 3)), dma((NCH,)), dma((NCH,))]
        return pl.pallas_call(
            kernel,
            out_shape=jax.ShapeDtypeStruct((TOK, D), BF16),
            in_specs=[hbm] * 11,
            out_specs=pl.BlockSpec(memory_space=pltpu.VMEM),
            scratch_shapes=scratch,
            compiler_params=pltpu.CompilerParams(collective_id=0, has_side_effects=True, vmem_limit_bytes=66_000_000),
            name="moe_layer",
        )(normed, residual, w_router.T, ws_gate, ws_up, ws_down, jnp.swapaxes(we_gate, 1, 2), jnp.swapaxes(we_up, 1, 2), we_down,
          first_id.reshape(1, TOK), alt_id.reshape(1, TOK))

    return jax.shard_map(device_step, mesh=mesh,
                         in_specs=(tok_spec, tok_spec, P(None, None), P(None, "tp"), P(None, "tp"), P("tp", None), P("ep", None, "tp"),
                                   P("ep", None, "tp"), P("ep", "tp", None), id_spec, id_spec),
                         out_specs=tok_spec, check_vma=False)
```

```python
import functools

import jax
import jax.numpy as jnp
from jax import lax
from jax.experimental import pallas as pl
from jax.experimental.pallas import tpu as pltpu
from jax.sharding import PartitionSpec as P

MESH = pl.DeviceIdType.MESH
scope = jax.named_scope
F32, BF16, I32 = jnp.float32, jnp.bfloat16, jnp.int32

EP = 4
TOK = 128
ALL = EP * TOK
EXPERTS = 64
LOCAL = EXPERTS // EP
CAP = 10
SLOT = 16
SLOTS = LOCAL * SLOT
PAIR = 64
D = 1280
FFE = 448
FFS = 896
GRP = 4
NGRP = LOCAL // GRP
KC = ((0, 512), (512, 512), (1024, 256))
NC = 256
NCH = D // NC


def nn(a, b):
    return lax.dot_general(a, b, (((1,), (0,)), ((), ())), preferred_element_type=F32)


def nt(a, b):
    return lax.dot_general(a, b, (((1,), (1,)), ((), ())), preferred_element_type=F32)


def silu_mul(g, u):
    return (g * (1.0 / (1.0 + jnp.exp(-g))) * u).astype(BF16)


def kernel(normed, residual, wr, wsg, wsu, wsd, weg, weu, wed, fid, aid, out_ref,
           x0, x1, x2, res_v, wr_v, fids, aids,
           sg, su, sd, w1g, w1u, w2g, w2u, w3g, w3u,
           xs0, xs1, xs2, accg, accu, hid, hid_s,
           sh_part, sh_recv, gmat, tmat, gcol, csend, crecv, ypart, yrecv, slot_out, obuf,
           x_sem, id_sem, misc_sem, sw_sem, w_sem, d_sem,
           xs_send, xs_recv, id_send, id_recv, sh_sem, c_send, c_recv, y_send, y_recv, o_sem):
    me = lax.axis_index("ep")
    tp = lax.axis_index("tp")
    xpeer = lax.rem(me + 2, EP)
    cpeer = me + 1 - 2 * lax.rem(me, 2)
    diag = lax.rem(cpeer + 2, EP)
    xr = (x0, x1, x2)
    xsr = (xs0, xs1, xs2)
    wgr, wur = (w1g, w2g, w3g), (w1u, w2u, w3u)
    mine = pl.ds(pl.multiple_of(me * TOK, TOK), TOK)

    def start(c):
        c.start()
        return c

    idc = [start(pltpu.make_async_copy(fid, fids.at[me], id_sem.at[0])),
           start(pltpu.make_async_copy(aid, aids.at[me], id_sem.at[1]))]
    xc = [start(pltpu.make_async_copy(normed.at[:, pl.ds(k, n)], xr[c].at[mine], x_sem.at[c])) for c, (k, n) in enumerate(KC)]
    wrc = start(pltpu.make_async_copy(wr, wr_v, misc_sem.at[0]))

    def gu_copy(p, g, i):
        k, n = KC[p]
        src = (weg, weu)[i].at[pl.ds(GRP * g, GRP), :, pl.ds(k, n)]
        return pltpu.make_async_copy(src, (wgr, wur)[i][p].at[pl.ds(GRP * g, GRP)], w_sem.at[p, g, i])

    def d_copy(j, g):
        ref, col = ((w1g, 0), (w1g, NC), (w1u, 0), (w1u, NC), (w2g, 0))[j]
        return pltpu.make_async_copy(wed.at[pl.ds(GRP * g, GRP), :, pl.ds(j * NC, NC)],
                                     ref.at[pl.ds(GRP * g, GRP), :, pl.ds(col, NC)], d_sem.at[j, g])

    def start_pass(p):
        for g in range(NGRP):
            for i in range(2):
                gu_copy(p, g, i).start()


    with scope("barrier"):
        bar = pltpu.get_barrier_semaphore()
        for o in (xpeer, cpeer, diag):
            pl.semaphore_signal(bar, inc=1, device_id={"ep": o}, device_id_type=MESH)
        pl.semaphore_signal(bar, inc=1, device_id={"tp": 1 - tp}, device_id_type=MESH)
        pl.semaphore_wait(bar, 4)

    sends = []

    def rcopy(src, dst, s, r, **dev):
        c = pltpu.make_async_remote_copy(src_ref=src, dst_ref=dst, send_sem=s, recv_sem=r, device_id=dev, device_id_type=MESH)
        c.start()
        sends.append(c)
        return c

    with scope("idload"):
        for c in idc:
            c.wait()
    idr = []
    for d in range(1, EP):
        o = lax.rem(me + d, EP)
        for i, ref in enumerate((fids, aids)):
            idr.append(rcopy(ref.at[me], ref.at[me], id_send.at[i, d - 1], id_recv.at[i, d - 1], ep=o))
    with scope("xsend"):
        xsend, csnd, fwd = [], [], []
        for c in range(3):
            xc[c].wait()
            xsend.append(rcopy(xr[c].at[mine], xr[c].at[mine], xs_send.at[0, c], xs_recv.at[0, c], ep=xpeer))
        for c in range(3):
            csnd.append(rcopy(xr[c].at[mine], xr[c].at[mine], xs_send.at[1, c], xs_recv.at[1, c], ep=cpeer))

    swc = [start(pltpu.make_async_copy(s, d, sw_sem.at[i])) for i, (s, d) in enumerate(((wsg, sg), (wsu, su), (wsd, sd)))]
    start_pass(0)
    resc = start(pltpu.make_async_copy(residual, res_v, misc_sem.at[1]))
    theirs = pl.ds(pl.multiple_of(xpeer * TOK, TOK), TOK)

    def forward(c):
        with scope(f"fwait{c}"):
            xsend[c].wait_recv()
        fwd.append(rcopy(xr[c].at[theirs], xr[c].at[theirs], xs_send.at[2, c], xs_recv.at[2, c], ep=cpeer))

    xo = [xr[c][mine, :] for c in range(3)]
    with scope("shwait"):
        swc[0].wait()
        swc[1].wait()
    with scope("shgu"):
        for n0 in range(0, FFS, 256):
            n = min(256, FFS - n0)
            g = sum(nn(xr[c][mine, :], sg[k:k + kn, n0:n0 + n]) for c, (k, kn) in enumerate(KC))
            u = sum(nn(xr[c][mine, :], su[k:k + kn, n0:n0 + n]) for c, (k, kn) in enumerate(KC))
            hid_s[:, n0:n0 + n] = silu_mul(g, u)
    with scope("shdown"):
        swc[2].wait()
        for n0 in range(0, D, 256):
            sh_part[:, n0:n0 + 256] = nn(hid_s[...], sd[:, n0:n0 + 256]).astype(BF16)
    start_pass(1)
    start_pass(2)

    with scope("router"):
        wrc.wait()
        wr_hi = wr_v[...].astype(BF16)
        wr_lo = (wr_v[...] - wr_hi.astype(F32)).astype(BF16)
        logits = jnp.zeros((TOK, EXPERTS), F32)
        for c, (k, kn) in enumerate(KC):
            logits = logits + nt(xo[c], wr_hi[:, k:k + kn]) + nt(xo[c], wr_lo[:, k:k + kn])
        ex = jnp.exp(logits - jnp.max(logits, axis=1, keepdims=True))
        prob = ex / jnp.sum(ex, axis=1, keepdims=True)
    shc = rcopy(sh_part, sh_recv, sh_sem.at[0], sh_sem.at[1], tp=1 - tp)

    with scope("idwait"):
        for c in idr:
            c.wait_recv()
    with scope("routing"):
        f = jnp.concatenate([fids[o] for o in range(EP)], axis=1)
        a = jnp.concatenate([aids[o] for o in range(EP)], axis=1)
        ti, tj = lax.broadcasted_iota(I32, (ALL, ALL), 0), lax.broadcasted_iota(I32, (ALL, ALL), 1)
        before = jnp.where(ti < tj, 1.0, 0.0)
        before_dev = jnp.where((ti // TOK) == (tj // TOK), before, 0.0).astype(BF16)
        before = before.astype(BF16)
        eio = lax.broadcasted_iota(I32, (EXPERTS, ALL), 0)
        one_f = jnp.where(eio == f, 1.0, 0.0)
        one_a = jnp.where(eio == a, 1.0, 0.0)
        rank_f = jnp.sum(nn(one_f.astype(BF16), before) * one_f, axis=0, keepdims=True)
        kept = rank_f < CAP - 0.5
        load = jnp.minimum(jnp.sum(one_f, axis=1, keepdims=True), float(CAP))
        over_a = one_a * jnp.where(kept, 0.0, 1.0)
        rank_a = jnp.sum(nn(over_a.astype(BF16), before) * over_a, axis=0, keepdims=True)
        load_a = jnp.sum(one_a * load, axis=0, keepdims=True)
        active = kept | (rank_a + load_a < CAP - 0.5)
        chosen = jnp.where(kept, f, a)
        slot = jnp.where(kept, rank_f, load_a + rank_a).astype(I32)
        owner = chosen // LOCAL
        local = chosen - owner * LOCAL
        here = active & (owner == me)
        slot_code = jnp.where(here, local * SLOT + slot, -1)
        oio = lax.broadcasted_iota(I32, (16, ALL), 0)
        own_f = jnp.where(oio == f // LOCAL, 1.0, 0.0)
        own_a = jnp.where(oio == a // LOCAL + EP, 1.0, 0.0)
        seen = nn((own_f + own_a).astype(BF16), before_dev)
        pos_f = jnp.sum(seen * own_f, axis=0, keepdims=True)
        pos_a = jnp.sum(seen * own_a, axis=0, keepdims=True)
        pos = jnp.where(kept, pos_f, pos_a + PAIR // 2).astype(I32)
        origin = lax.broadcasted_iota(I32, (1, ALL), 1) // TOK
        pair_code = jnp.where(here, origin * PAIR + pos, -1)
        back_code = jnp.where(active, owner * PAIR + pos, -1)
        sio = lax.broadcasted_iota(I32, (SLOTS, ALL), 0)
        smat = jnp.where(sio == slot_code, 1.0, 0.0).astype(BF16)
        rmat = jnp.where(sio == pair_code, 1.0, 0.0).astype(BF16)
        gmat[...] = nt(rmat, smat).astype(BF16)

        own_back, own_chosen = back_code[:, :TOK], jnp.where(active, chosen, -1)[:, :TOK]
        all_chosen = jnp.where(active, chosen, -1)
        for o in range(1, EP):
            cols = slice(o * TOK, (o + 1) * TOK)
            own_back = jnp.where(me == o, back_code[:, cols], own_back)
            own_chosen = jnp.where(me == o, all_chosen[:, cols], own_chosen)
        eye = jnp.where(lax.broadcasted_iota(I32, (TOK, TOK), 0) == lax.broadcasted_iota(I32, (TOK, TOK), 1), 1.0, 0.0).astype(BF16)
        bio = lax.broadcasted_iota(I32, (EP * PAIR, TOK), 0)
        tmat[...] = nt(eye, jnp.where(bio == own_back, 1.0, 0.0).astype(BF16)).astype(BF16)
        cio = lax.broadcasted_iota(I32, (EXPERTS, TOK), 0)
        pick = nt(eye, jnp.where(cio == own_chosen, 1.0, 0.0).astype(BF16))
        gcol[...] = jnp.sum(prob * pick, axis=1, keepdims=True)

    def gather(c):
        with scope(f"xwait{c}"):
            csnd[c].wait_recv()
            fwd[c].wait_recv()
        with scope(f"gather{c}"):
            xsr[c][...] = nn(smat, xr[c][...]).astype(BF16)

    def gu_pass(p, lo, hi):
        @pl.loop(lo, hi)
        def _(g):
            with scope(f"ww{p}"):
                gu_copy(p, g, 0).wait()
                gu_copy(p, g, 1).wait()
            for i in range(GRP):
                e = g * GRP + i
                rows = pl.ds(pl.multiple_of(e * SLOT, SLOT), SLOT)
                xe = xsr[p][rows, :]
                dg, du = nt(xe, wgr[p][e]), nt(xe, wur[p][e])
                if p == 0:
                    accg[rows, :] = dg
                    accu[rows, :] = du
                elif p == 1:
                    accg[rows, :] += dg
                    accu[rows, :] += du
                else:
                    hid[rows, :] = silu_mul(accg[rows, :] + dg, accu[rows, :] + du)

    forward(0)
    gather(0)
    gu_pass(0, 0, NGRP)
    forward(1)
    for j in range(NCH - 1):
        for g in range(NGRP):
            d_copy(j, g).start()
    gather(1)
    gu_pass(1, 0, 2)
    forward(2)
    gu_pass(1, 2, NGRP)
    for g in range(NGRP):
        d_copy(NCH - 1, g).start()
    gather(2)
    gu_pass(2, 0, NGRP)

    cr, yr = [], []

    def exchange(j):
        with scope(f"cw{j}"):
            for c in cr[j]:
                c.wait_recv()
        ypart[j] = nn(tmat[...], crecv[j]).astype(BF16)
        yr.append(rcopy(ypart.at[j], yrecv.at[j], y_send.at[j], y_recv.at[j], tp=1 - tp))

    my_rows = pl.ds(pl.multiple_of(me * PAIR, PAIR), PAIR)
    for j in range(NCH):
        ref, col = ((w1g, 0), (w1g, NC), (w1u, 0), (w1u, NC), (w2g, 0))[j]

        @pl.loop(0, NGRP)
        def _(g):
            with scope(f"dw{j}"):
                d_copy(j, g).wait()
            for i in range(GRP):
                e = g * GRP + i
                rows = pl.ds(pl.multiple_of(e * SLOT, SLOT), SLOT)
                slot_out[rows, :] = nn(hid[rows, :], ref[e, :, col:col + NC]).astype(BF16)

        with scope(f'gx{j}'):
            csend[j] = nn(gmat[...], slot_out[...]).astype(BF16)
        crecv[j, my_rows, :] = csend[j, my_rows, :]
        row = []
        for d in range(1, EP):
            o = lax.rem(me + d, EP)
            row.append(rcopy(csend.at[j, pl.ds(pl.multiple_of(o * PAIR, PAIR), PAIR)], crecv.at[j, my_rows],
                             c_send.at[j, d - 1], c_recv.at[j, d - 1], ep=o))
        cr.append(row)
        if j >= 2:
            exchange(j - 2)

    exchange(NCH - 2)
    exchange(NCH - 1)
    resc.wait()
    shc.wait_recv()
    oc = []
    for j in range(NCH):
        cols = slice(j * NC, (j + 1) * NC)
        base = res_v[:, cols].astype(F32) + (sh_part[:, cols].astype(F32) + sh_recv[:, cols].astype(F32))
        with scope(f"yw{j}"):
            yr[j].wait_recv()
        routed = (ypart[j].astype(F32) + yrecv[j].astype(F32)).astype(BF16).astype(F32)
        obuf[:, cols] = (base + gcol[...] * routed).astype(BF16)
        oc.append(start(pltpu.make_async_copy(obuf.at[:, pl.ds(j * NC, NC)], out_ref.at[:, pl.ds(j * NC, NC)], o_sem.at[j])))
    with scope('sendwait'):
        for c in sends:
            c.wait_send()
    with scope('outwait'):
        for c in oc:
            c.wait()


def solution(mesh):
    tok_spec, id_spec = P(("dp", "ep"), None), P(("dp", "ep"))

    def device_step(normed, residual, w_router, ws_gate, ws_up, ws_down, we_gate, we_up, we_down, first_id, alt_id):
        hbm = pl.BlockSpec(memory_space=pl.ANY)
        vm, dma = pltpu.VMEM, pltpu.SemaphoreType.DMA
        weights = [vm((LOCAL, FFE, n), BF16) for _, n in KC for _ in range(2)]
        scratch = [vm((ALL, n), BF16) for _, n in KC]
        scratch += [vm((TOK, D), BF16), vm((EXPERTS, D), F32), vm((EP, 1, TOK), I32), vm((EP, 1, TOK), I32)]
        scratch += [vm((D, FFS), BF16), vm((D, FFS), BF16), vm((FFS, D), BF16)] + weights
        scratch += [vm((SLOTS, n), BF16) for _, n in KC]
        scratch += [vm((SLOTS, FFE), F32), vm((SLOTS, FFE), F32), vm((SLOTS, FFE), BF16), vm((TOK, FFS), BF16)]
        scratch += [vm((TOK, D), BF16), vm((TOK, D), BF16), vm((EP * PAIR, SLOTS), BF16), vm((TOK, EP * PAIR), BF16), vm((TOK, 1), F32)]
        scratch += [vm((NCH, EP * PAIR, NC), BF16), vm((NCH, EP * PAIR, NC), BF16), vm((NCH, TOK, NC), BF16), vm((NCH, TOK, NC), BF16), vm((SLOTS, NC), BF16), vm((TOK, D), BF16)]
        scratch += [dma((3,)), dma((2,)), dma((2,)), dma((3,)), dma((3, NGRP, 2)), dma((NCH, NGRP)),
                    dma((3, 3)), dma((3, 3)), dma((2, 3)), dma((2, 3)), dma((2,)), dma((NCH, 3)), dma((NCH, 3)), dma((NCH,)), dma((NCH,)), dma((NCH,))]
        return pl.pallas_call(
            kernel,
            out_shape=jax.ShapeDtypeStruct((TOK, D), BF16),
            in_specs=[hbm] * 11,
            out_specs=hbm,
            scratch_shapes=scratch,
            compiler_params=pltpu.CompilerParams(collective_id=0, has_side_effects=True, vmem_limit_bytes=66_000_000),
            name="moe_layer",
        )(normed, residual, w_router.T, ws_gate, ws_up, ws_down, jnp.swapaxes(we_gate, 1, 2), jnp.swapaxes(we_up, 1, 2), we_down,
          first_id.reshape(1, TOK), alt_id.reshape(1, TOK))

    return jax.shard_map(device_step, mesh=mesh,
                         in_specs=(tok_spec, tok_spec, P(None, None), P(None, "tp"), P(None, "tp"), P("tp", None), P("ep", None, "tp"),
                                   P("ep", None, "tp"), P("ep", "tp", None), id_spec, id_spec),
                         out_specs=tok_spec, check_vma=False)
```

```python
import functools

import jax
import jax.numpy as jnp
from jax import lax
from jax.experimental import pallas as pl
from jax.experimental.pallas import tpu as pltpu
from jax.sharding import PartitionSpec as P

MESH = pl.DeviceIdType.MESH
scope = jax.named_scope
F32, BF16, I32 = jnp.float32, jnp.bfloat16, jnp.int32

EP = 4
TOK = 128
ALL = EP * TOK
EXPERTS = 64
LOCAL = EXPERTS // EP
CAP = 10
SLOT = 16
SLOTS = LOCAL * SLOT
PAIR = 64
D = 1280
FFE = 448
FFS = 896
GRP = 4
NGRP = LOCAL // GRP
KC = ((0, 256), (256, 512), (768, 512))
NC = 256
NCH = D // NC
LAG = 3


def nn(a, b):
    return lax.dot_general(a, b, (((1,), (0,)), ((), ())), preferred_element_type=F32)


def nt(a, b):
    return lax.dot_general(a, b, (((1,), (1,)), ((), ())), preferred_element_type=F32)


def silu_mul(g, u):
    return (g * (1.0 / (1.0 + jnp.exp(-g))) * u).astype(BF16)


def kernel(normed, residual, wr, wsg, wsu, wsd, weg, weu, wed, fid, aid, out_ref,
           x0, x1, x2, res_v, wr_v, fids, aids,
           sg, su, sd, w1g, w1u, w2g, w2u, w3g, w3u,
           xs0, xs1, xs2, accg, accu, hid, hid_s,
           sh_part, sh_recv, gmat, tmat, gcol, csend, crecv, ypart, yrecv, slot_out, obuf,
           x_sem, id_sem, misc_sem, sw_sem, w_sem, d_sem,
           xs_send, xs_recv, id_send, id_recv, sh_sem, c_send, c_recv, y_send, y_recv, o_sem):
    me = lax.axis_index("ep")
    tp = lax.axis_index("tp")
    xpeer = lax.rem(me + 2, EP)
    cpeer = me + 1 - 2 * lax.rem(me, 2)
    diag = lax.rem(cpeer + 2, EP)
    xr = (x0, x1, x2)
    xsr = (xs0, xs1, xs2)
    wgr, wur = (w1g, w2g, w3g), (w1u, w2u, w3u)
    mine = pl.ds(pl.multiple_of(me * TOK, TOK), TOK)

    def start(c):
        c.start()
        return c

    idc = [start(pltpu.make_async_copy(fid, fids.at[me], id_sem.at[0])),
           start(pltpu.make_async_copy(aid, aids.at[me], id_sem.at[1]))]
    xc = [start(pltpu.make_async_copy(normed.at[:, pl.ds(k, n)], xr[c].at[mine], x_sem.at[c])) for c, (k, n) in enumerate(KC)]
    wrc = start(pltpu.make_async_copy(wr, wr_v, misc_sem.at[0]))

    def gu_copy(p, g, i):
        k, n = KC[p]
        src = (weg, weu)[i].at[pl.ds(GRP * g, GRP), :, pl.ds(k, n)]
        return pltpu.make_async_copy(src, (wgr, wur)[i][p].at[pl.ds(GRP * g, GRP)], w_sem.at[p, g, i])

    def d_copy(j, g):
        ref, col = ((w1g, 0), (w1u, 0), (w2g, 0), (w2g, NC), (w2u, 0))[j]
        return pltpu.make_async_copy(wed.at[pl.ds(GRP * g, GRP), :, pl.ds(j * NC, NC)],
                                     ref.at[pl.ds(GRP * g, GRP), :, pl.ds(col, NC)], d_sem.at[j, g])

    def start_down(j):
        for g in range(NGRP):
            d_copy(j, g).start()

    def start_pass(p):
        for g in range(NGRP):
            for i in range(2):
                gu_copy(p, g, i).start()


    with scope("barrier"):
        bar = pltpu.get_barrier_semaphore()
        for o in (xpeer, cpeer, diag):
            pl.semaphore_signal(bar, inc=1, device_id={"ep": o}, device_id_type=MESH)
        pl.semaphore_signal(bar, inc=1, device_id={"tp": 1 - tp}, device_id_type=MESH)
        for c in idc + xc:
            c.wait()
        swc = [start(pltpu.make_async_copy(s, d, sw_sem.at[i])) for i, (s, d) in enumerate(((wsg, sg), (wsu, su), (wsd, sd)))]
        pl.semaphore_wait(bar, 4)

    sends = []

    def rcopy(src, dst, s, r, **dev):
        c = pltpu.make_async_remote_copy(src_ref=src, dst_ref=dst, send_sem=s, recv_sem=r, device_id=dev, device_id_type=MESH)
        c.start()
        sends.append(c)
        return c

    idr = []
    for d in range(1, EP):
        o = lax.rem(me + d, EP)
        for i, ref in enumerate((fids, aids)):
            idr.append(rcopy(ref.at[me], ref.at[me], id_send.at[i, d - 1], id_recv.at[i, d - 1], ep=o))
    with scope("xsend"):
        xsend, csnd, fwd = [], [], []
        for c in range(3):
            xsend.append(rcopy(xr[c].at[mine], xr[c].at[mine], xs_send.at[0, c], xs_recv.at[0, c], ep=xpeer))
        for c in range(3):
            csnd.append(rcopy(xr[c].at[mine], xr[c].at[mine], xs_send.at[1, c], xs_recv.at[1, c], ep=cpeer))

    theirs = pl.ds(pl.multiple_of(xpeer * TOK, TOK), TOK)

    def forward(c):
        with scope(f"fwait{c}"):
            xsend[c].wait_recv()
        fwd.append(rcopy(xr[c].at[theirs], xr[c].at[theirs], xs_send.at[2, c], xs_recv.at[2, c], ep=cpeer))

    xo = [xr[c][mine, :] for c in range(3)]
    with scope("shwait"):
        swc[0].wait()
        swc[1].wait()
    start_pass(0)
    resc = start(pltpu.make_async_copy(residual, res_v, misc_sem.at[1]))
    with scope("shgu"):
        for n0 in range(0, FFS, 256):
            n = min(256, FFS - n0)
            g = sum(nn(xr[c][mine, :], sg[k:k + kn, n0:n0 + n]) for c, (k, kn) in enumerate(KC))
            u = sum(nn(xr[c][mine, :], su[k:k + kn, n0:n0 + n]) for c, (k, kn) in enumerate(KC))
            hid_s[:, n0:n0 + n] = silu_mul(g, u)
    with scope("shdown"):
        swc[2].wait()
        for n0 in range(0, D, 256):
            sh_part[:, n0:n0 + 256] = nn(hid_s[...], sd[:, n0:n0 + 256]).astype(BF16)
    start_pass(1)
    start_pass(2)

    forward(0)
    with scope("router"):
        wrc.wait()
        wr_hi = wr_v[...].astype(BF16)
        wr_lo = (wr_v[...] - wr_hi.astype(F32)).astype(BF16)
        logits = jnp.zeros((TOK, EXPERTS), F32)
        for c, (k, kn) in enumerate(KC):
            logits = logits + nt(xo[c], wr_hi[:, k:k + kn]) + nt(xo[c], wr_lo[:, k:k + kn])
        ex = jnp.exp(logits - jnp.max(logits, axis=1, keepdims=True))
        prob = ex / jnp.sum(ex, axis=1, keepdims=True)
    shc = rcopy(sh_part, sh_recv, sh_sem.at[0], sh_sem.at[1], tp=1 - tp)

    with scope("idwait"):
        for c in idr:
            c.wait_recv()
    with scope("routing"):
        f = jnp.concatenate([fids[o] for o in range(EP)], axis=1)
        a = jnp.concatenate([aids[o] for o in range(EP)], axis=1)
        ti, tj = lax.broadcasted_iota(I32, (ALL, ALL), 0), lax.broadcasted_iota(I32, (ALL, ALL), 1)
        before = jnp.where(ti < tj, 1.0, 0.0)
        before_dev = jnp.where((ti // TOK) == (tj // TOK), before, 0.0).astype(BF16)
        before = before.astype(BF16)
        eio = lax.broadcasted_iota(I32, (EXPERTS, ALL), 0)
        one_f = jnp.where(eio == f, 1.0, 0.0)
        one_a = jnp.where(eio == a, 1.0, 0.0)
        rank_f = jnp.sum(nn(one_f.astype(BF16), before) * one_f, axis=0, keepdims=True)
        kept = rank_f < CAP - 0.5
        load = jnp.minimum(jnp.sum(one_f, axis=1, keepdims=True), float(CAP))
        over_a = one_a * jnp.where(kept, 0.0, 1.0)
        rank_a = jnp.sum(nn(over_a.astype(BF16), before) * over_a, axis=0, keepdims=True)
        load_a = jnp.sum(one_a * load, axis=0, keepdims=True)
        active = kept | (rank_a + load_a < CAP - 0.5)
        chosen = jnp.where(kept, f, a)
        slot = jnp.where(kept, rank_f, load_a + rank_a).astype(I32)
        owner = chosen // LOCAL
        local = chosen - owner * LOCAL
        here = active & (owner == me)
        slot_code = jnp.where(here, local * SLOT + slot, -1)
        oio = lax.broadcasted_iota(I32, (16, ALL), 0)
        own_f = jnp.where(oio == f // LOCAL, 1.0, 0.0)
        own_a = jnp.where(oio == a // LOCAL + EP, 1.0, 0.0)
        seen = nn((own_f + own_a).astype(BF16), before_dev)
        pos_f = jnp.sum(seen * own_f, axis=0, keepdims=True)
        pos_a = jnp.sum(seen * own_a, axis=0, keepdims=True)
        pos = jnp.where(kept, pos_f, pos_a + PAIR // 2).astype(I32)
        origin = lax.broadcasted_iota(I32, (1, ALL), 1) // TOK
        pair_code = jnp.where(here, origin * PAIR + pos, -1)
        back_code = jnp.where(active, owner * PAIR + pos, -1)
        sio = lax.broadcasted_iota(I32, (SLOTS, ALL), 0)
        smat = jnp.where(sio == slot_code, 1.0, 0.0).astype(BF16)
        rmat = jnp.where(sio == pair_code, 1.0, 0.0).astype(BF16)
        gmat[...] = nt(rmat, smat).astype(BF16)

        own_back, own_chosen = back_code[:, :TOK], jnp.where(active, chosen, -1)[:, :TOK]
        all_chosen = jnp.where(active, chosen, -1)
        for o in range(1, EP):
            cols = slice(o * TOK, (o + 1) * TOK)
            own_back = jnp.where(me == o, back_code[:, cols], own_back)
            own_chosen = jnp.where(me == o, all_chosen[:, cols], own_chosen)
        eye = jnp.where(lax.broadcasted_iota(I32, (TOK, TOK), 0) == lax.broadcasted_iota(I32, (TOK, TOK), 1), 1.0, 0.0).astype(BF16)
        bio = lax.broadcasted_iota(I32, (EP * PAIR, TOK), 0)
        tmat[...] = nt(eye, jnp.where(bio == own_back, 1.0, 0.0).astype(BF16)).astype(BF16)
        cio = lax.broadcasted_iota(I32, (EXPERTS, TOK), 0)
        pick = nt(eye, jnp.where(cio == own_chosen, 1.0, 0.0).astype(BF16))
        gcol[...] = jnp.sum(prob * pick, axis=1, keepdims=True)

    def gather(c):
        with scope(f"xwait{c}"):
            csnd[c].wait_recv()
            fwd[c].wait_recv()
        with scope(f"gather{c}"):
            xsr[c][...] = nn(smat, xr[c][...]).astype(BF16)

    def gu_pass(p, lo, hi):
        @pl.loop(lo, hi)
        def _(g):
            with scope(f"ww{p}"):
                gu_copy(p, g, 0).wait()
                gu_copy(p, g, 1).wait()
            for i in range(GRP):
                e = g * GRP + i
                rows = pl.ds(pl.multiple_of(e * SLOT, SLOT), SLOT)
                xe = xsr[p][rows, :]
                dg, du = nt(xe, wgr[p][e]), nt(xe, wur[p][e])
                if p == 0:
                    accg[rows, :] = dg
                    accu[rows, :] = du
                elif p == 1:
                    accg[rows, :] += dg
                    accu[rows, :] += du
                else:
                    hid[rows, :] = silu_mul(accg[rows, :] + dg, accu[rows, :] + du)

    gather(0)
    gu_pass(0, 0, 3)
    forward(1)
    gu_pass(0, 3, NGRP)
    start_down(0)
    start_down(1)
    gather(1)
    gu_pass(1, 0, 1)
    forward(2)
    gu_pass(1, 1, NGRP)
    for j in range(2, NCH):
        start_down(j)
    gather(2)
    gu_pass(2, 0, NGRP)

    cr, yr = [], []

    def exchange(j):
        with scope(f"cw{j}"):
            for c in cr[j]:
                c.wait_recv()
        ypart[j] = nn(tmat[...], crecv[j]).astype(BF16)
        yr.append(rcopy(ypart.at[j], yrecv.at[j], y_send.at[j], y_recv.at[j], tp=1 - tp))

    my_rows = pl.ds(pl.multiple_of(me * PAIR, PAIR), PAIR)
    for j in range(NCH):
        ref, col = ((w1g, 0), (w1u, 0), (w2g, 0), (w2g, NC), (w2u, 0))[j]

        @pl.loop(0, NGRP)
        def _(g):
            with scope(f"dw{j}"):
                d_copy(j, g).wait()
            for i in range(GRP):
                e = g * GRP + i
                rows = pl.ds(pl.multiple_of(e * SLOT, SLOT), SLOT)
                slot_out[rows, :] = nn(hid[rows, :], ref[e, :, col:col + NC]).astype(BF16)

        with scope(f'gx{j}'):
            csend[j] = nn(gmat[...], slot_out[...]).astype(BF16)
        crecv[j, my_rows, :] = csend[j, my_rows, :]
        row = []
        for d in range(1, EP):
            o = lax.rem(me + d, EP)
            row.append(rcopy(csend.at[j, pl.ds(pl.multiple_of(o * PAIR, PAIR), PAIR)], crecv.at[j, my_rows],
                             c_send.at[j, d - 1], c_recv.at[j, d - 1], ep=o))
        cr.append(row)
        if j >= LAG:
            exchange(j - LAG)

    for j in range(NCH - LAG, NCH):
        exchange(j)
    resc.wait()
    shc.wait_recv()
    oc = []
    for j in range(NCH):
        cols = slice(j * NC, (j + 1) * NC)
        base = res_v[:, cols].astype(F32) + (sh_part[:, cols].astype(F32) + sh_recv[:, cols].astype(F32))
        with scope(f"yw{j}"):
            yr[j].wait_recv()
        routed = (ypart[j].astype(F32) + yrecv[j].astype(F32)).astype(BF16).astype(F32)
        obuf[:, cols] = (base + gcol[...] * routed).astype(BF16)
        oc.append(start(pltpu.make_async_copy(obuf.at[:, pl.ds(j * NC, NC)], out_ref.at[:, pl.ds(j * NC, NC)], o_sem.at[j])))
    with scope('sendwait'):
        for c in sends:
            c.wait_send()
    with scope('outwait'):
        for c in oc:
            c.wait()


def solution(mesh):
    tok_spec, id_spec = P(("dp", "ep"), None), P(("dp", "ep"))

    def device_step(normed, residual, w_router, ws_gate, ws_up, ws_down, we_gate, we_up, we_down, first_id, alt_id):
        hbm = pl.BlockSpec(memory_space=pl.ANY)
        vm, dma = pltpu.VMEM, pltpu.SemaphoreType.DMA
        weights = [vm((LOCAL, FFE, n), BF16) for _, n in KC for _ in range(2)]
        scratch = [vm((ALL, n), BF16) for _, n in KC]
        scratch += [vm((TOK, D), BF16), vm((EXPERTS, D), F32), vm((EP, 1, TOK), I32), vm((EP, 1, TOK), I32)]
        scratch += [vm((D, FFS), BF16), vm((D, FFS), BF16), vm((FFS, D), BF16)] + weights
        scratch += [vm((SLOTS, n), BF16) for _, n in KC]
        scratch += [vm((SLOTS, FFE), F32), vm((SLOTS, FFE), F32), vm((SLOTS, FFE), BF16), vm((TOK, FFS), BF16)]
        scratch += [vm((TOK, D), BF16), vm((TOK, D), BF16), vm((EP * PAIR, SLOTS), BF16), vm((TOK, EP * PAIR), BF16), vm((TOK, 1), F32)]
        scratch += [vm((NCH, EP * PAIR, NC), BF16), vm((NCH, EP * PAIR, NC), BF16), vm((NCH, TOK, NC), BF16), vm((NCH, TOK, NC), BF16), vm((SLOTS, NC), BF16), vm((TOK, D), BF16)]
        scratch += [dma((3,)), dma((2,)), dma((2,)), dma((3,)), dma((3, NGRP, 2)), dma((NCH, NGRP)),
                    dma((3, 3)), dma((3, 3)), dma((2, 3)), dma((2, 3)), dma((2,)), dma((NCH, 3)), dma((NCH, 3)), dma((NCH,)), dma((NCH,)), dma((NCH,))]
        return pl.pallas_call(
            kernel,
            out_shape=jax.ShapeDtypeStruct((TOK, D), BF16),
            in_specs=[hbm] * 11,
            out_specs=hbm,
            scratch_shapes=scratch,
            compiler_params=pltpu.CompilerParams(collective_id=0, has_side_effects=True, vmem_limit_bytes=66_000_000),
            name="moe_layer",
        )(normed, residual, w_router.T, ws_gate, ws_up, ws_down, jnp.swapaxes(we_gate, 1, 2), jnp.swapaxes(we_up, 1, 2), we_down,
          first_id.reshape(1, TOK), alt_id.reshape(1, TOK))

    return jax.shard_map(device_step, mesh=mesh,
                         in_specs=(tok_spec, tok_spec, P(None, None), P(None, "tp"), P(None, "tp"), P("tp", None), P("ep", None, "tp"),
                                   P("ep", None, "tp"), P("ep", "tp", None), id_spec, id_spec),
                         out_specs=tok_spec, check_vma=False)
```

```python
import functools

import jax
import jax.numpy as jnp
from jax import lax
from jax.experimental import pallas as pl
from jax.experimental.pallas import tpu as pltpu
from jax.sharding import PartitionSpec as P

MESH = pl.DeviceIdType.MESH
scope = jax.named_scope
F32, BF16, I32 = jnp.float32, jnp.bfloat16, jnp.int32

EP = 4
TOK = 128
ALL = EP * TOK
EXPERTS = 64
LOCAL = EXPERTS // EP
CAP = 10
SLOT = 16
SLOTS = LOCAL * SLOT
PAIR = 64
D = 1280
FFE = 448
FFS = 896
GRP = 4
NGRP = LOCAL // GRP
KC = ((0, 256), (256, 512), (768, 512))
NC = 256
NCH = D // NC
LAG = 3


def nn(a, b):
    return lax.dot_general(a, b, (((1,), (0,)), ((), ())), preferred_element_type=F32)


def nt(a, b):
    return lax.dot_general(a, b, (((1,), (1,)), ((), ())), preferred_element_type=F32)


def silu_mul(g, u):
    return (g * (1.0 / (1.0 + jnp.exp(-g))) * u).astype(BF16)


def kernel(normed, residual, wr, wsg, wsu, wsd, weg, weu, wed, fid, aid, out_ref,
           x0, x1, x2, res_v, wr_v, fids, aids,
           sg, su, sd, w1g, w1u, w2g, w2u, w3g, w3u,
           xs0, xs1, xs2, accg, accu, hid, hid_s,
           sh_part, sh_recv, gmat, tmat, gcol, csend, crecv, ypart, yrecv, slot_out, obuf, wt0, wt1,
           x_sem, id_sem, misc_sem, sw_sem, w_sem, d_sem,
           xs_send, xs_recv, id_send, id_recv, sh_sem, c_send, c_recv, y_send, y_recv, o_sem):
    me = lax.axis_index("ep")
    tp = lax.axis_index("tp")
    xpeer = lax.rem(me + 2, EP)
    cpeer = me + 1 - 2 * lax.rem(me, 2)
    diag = lax.rem(cpeer + 2, EP)
    xr = (x0, x1, x2)
    xsr = (xs0, xs1, xs2)
    wgr, wur = (w1g, w2g, w3g), (w1u, w2u, w3u)
    mine = pl.ds(pl.multiple_of(me * TOK, TOK), TOK)

    def start(c):
        c.start()
        return c

    idc = [start(pltpu.make_async_copy(fid, fids.at[me], id_sem.at[0])),
           start(pltpu.make_async_copy(aid, aids.at[me], id_sem.at[1]))]
    xc = [start(pltpu.make_async_copy(normed.at[:, pl.ds(k, n)], xr[c].at[mine], x_sem.at[c])) for c, (k, n) in enumerate(KC)]
    wrc = start(pltpu.make_async_copy(wr, wr_v, misc_sem.at[0]))

    def gu_copy(p, g, i):
        k, n = KC[p]
        src = (weg, weu)[i].at[pl.ds(GRP * g, GRP), :, pl.ds(k, n)]
        return pltpu.make_async_copy(src, (wgr, wur)[i][p].at[pl.ds(GRP * g, GRP)], w_sem.at[p, g, i])

    def d_copy(j, g):
        ref, col = ((w1u, 0), (w2g, 0), (w2g, NC), (w2u, 0), (w1g, 0))[j]
        return pltpu.make_async_copy(wed.at[pl.ds(GRP * g, GRP), :, pl.ds(j * NC, NC)],
                                     ref.at[pl.ds(GRP * g, GRP), :, pl.ds(col, NC)], d_sem.at[j, g])

    def start_down(j):
        for g in range(NGRP):
            d_copy(j, g).start()

    def start_pass(p):
        for g in range(NGRP):
            for i in range(2):
                gu_copy(p, g, i).start()


    with scope("barrier"):
        bar = pltpu.get_barrier_semaphore()
        for o in (xpeer, cpeer, diag):
            pl.semaphore_signal(bar, inc=1, device_id={"ep": o}, device_id_type=MESH)
        pl.semaphore_signal(bar, inc=1, device_id={"tp": 1 - tp}, device_id_type=MESH)
        for c in idc + xc:
            c.wait()
        swc = [start(pltpu.make_async_copy(s, d, sw_sem.at[i])) for i, (s, d) in enumerate(((wsg, sg), (wsu, su), (wsd, sd)))]
        pl.semaphore_wait(bar, 4)

    sends = []

    def rcopy(src, dst, s, r, **dev):
        c = pltpu.make_async_remote_copy(src_ref=src, dst_ref=dst, send_sem=s, recv_sem=r, device_id=dev, device_id_type=MESH)
        c.start()
        sends.append(c)
        return c

    idr = []
    for d in range(1, EP):
        o = lax.rem(me + d, EP)
        for i, ref in enumerate((fids, aids)):
            idr.append(rcopy(ref.at[me], ref.at[me], id_send.at[i, d - 1], id_recv.at[i, d - 1], ep=o))
    with scope("xsend"):
        xsend, csnd, fwd = [], [], []
        for c in range(3):
            xsend.append(rcopy(xr[c].at[mine], xr[c].at[mine], xs_send.at[0, c], xs_recv.at[0, c], ep=xpeer))
        for c in range(3):
            csnd.append(rcopy(xr[c].at[mine], xr[c].at[mine], xs_send.at[1, c], xs_recv.at[1, c], ep=cpeer))

    theirs = pl.ds(pl.multiple_of(xpeer * TOK, TOK), TOK)

    def forward(c):
        with scope(f"fwait{c}"):
            xsend[c].wait_recv()
        fwd.append(rcopy(xr[c].at[theirs], xr[c].at[theirs], xs_send.at[2, c], xs_recv.at[2, c], ep=cpeer))

    xo = [xr[c][mine, :] for c in range(3)]
    with scope("shwait"):
        swc[0].wait()
        swc[1].wait()
    start_pass(0)
    resc = start(pltpu.make_async_copy(residual, res_v, misc_sem.at[1]))
    with scope("shgu"):
        for n0 in range(0, FFS, 256):
            n = min(256, FFS - n0)
            g = sum(nn(xr[c][mine, :], sg[k:k + kn, n0:n0 + n]) for c, (k, kn) in enumerate(KC))
            u = sum(nn(xr[c][mine, :], su[k:k + kn, n0:n0 + n]) for c, (k, kn) in enumerate(KC))
            hid_s[:, n0:n0 + n] = silu_mul(g, u)
    with scope("shdown"):
        swc[2].wait()
        for n0 in range(0, D, 256):
            sh_part[:, n0:n0 + 256] = nn(hid_s[...], sd[:, n0:n0 + 256]).astype(BF16)
    start_pass(1)
    start_pass(2)

    forward(0)
    with scope("router"):
        wrc.wait()
        wr_hi = wr_v[...].astype(BF16)
        wr_lo = (wr_v[...] - wr_hi.astype(F32)).astype(BF16)
        logits = jnp.zeros((TOK, EXPERTS), F32)
        for c, (k, kn) in enumerate(KC):
            logits = logits + nt(xo[c], wr_hi[:, k:k + kn]) + nt(xo[c], wr_lo[:, k:k + kn])
        ex = jnp.exp(logits - jnp.max(logits, axis=1, keepdims=True))
        prob = ex / jnp.sum(ex, axis=1, keepdims=True)
    shc = rcopy(sh_part, sh_recv, sh_sem.at[0], sh_sem.at[1], tp=1 - tp)

    with scope("idwait"):
        for c in idr:
            c.wait_recv()
    with scope("routing"):
        f = jnp.concatenate([fids[o] for o in range(EP)], axis=1)
        a = jnp.concatenate([aids[o] for o in range(EP)], axis=1)
        ti, tj = lax.broadcasted_iota(I32, (ALL, ALL), 0), lax.broadcasted_iota(I32, (ALL, ALL), 1)
        before = jnp.where(ti < tj, 1.0, 0.0)
        before_dev = jnp.where((ti // TOK) == (tj // TOK), before, 0.0).astype(BF16)
        before = before.astype(BF16)
        eio = lax.broadcasted_iota(I32, (EXPERTS, ALL), 0)
        one_f = jnp.where(eio == f, 1.0, 0.0)
        one_a = jnp.where(eio == a, 1.0, 0.0)
        rank_f = jnp.sum(nn(one_f.astype(BF16), before) * one_f, axis=0, keepdims=True)
        kept = rank_f < CAP - 0.5
        load = jnp.minimum(jnp.sum(one_f, axis=1, keepdims=True), float(CAP))
        over_a = one_a * jnp.where(kept, 0.0, 1.0)
        rank_a = jnp.sum(nn(over_a.astype(BF16), before) * over_a, axis=0, keepdims=True)
        load_a = jnp.sum(one_a * load, axis=0, keepdims=True)
        active = kept | (rank_a + load_a < CAP - 0.5)
        chosen = jnp.where(kept, f, a)
        slot = jnp.where(kept, rank_f, load_a + rank_a).astype(I32)
        owner = chosen // LOCAL
        local = chosen - owner * LOCAL
        here = active & (owner == me)
        slot_code = jnp.where(here, local * SLOT + slot, -1)
        oio = lax.broadcasted_iota(I32, (16, ALL), 0)
        own_f = jnp.where(oio == f // LOCAL, 1.0, 0.0)
        own_a = jnp.where(oio == a // LOCAL + EP, 1.0, 0.0)
        seen = nn((own_f + own_a).astype(BF16), before_dev)
        pos_f = jnp.sum(seen * own_f, axis=0, keepdims=True)
        pos_a = jnp.sum(seen * own_a, axis=0, keepdims=True)
        pos = jnp.where(kept, pos_f, pos_a + PAIR // 2).astype(I32)
        origin = lax.broadcasted_iota(I32, (1, ALL), 1) // TOK
        pair_code = jnp.where(here, origin * PAIR + pos, -1)
        back_code = jnp.where(active, owner * PAIR + pos, -1)
        sio = lax.broadcasted_iota(I32, (SLOTS, ALL), 0)
        smat = jnp.where(sio == slot_code, 1.0, 0.0).astype(BF16)
        rmat = jnp.where(sio == pair_code, 1.0, 0.0).astype(BF16)
        gmat[...] = nt(rmat, smat).astype(BF16)

        own_back, own_chosen = back_code[:, :TOK], jnp.where(active, chosen, -1)[:, :TOK]
        all_chosen = jnp.where(active, chosen, -1)
        for o in range(1, EP):
            cols = slice(o * TOK, (o + 1) * TOK)
            own_back = jnp.where(me == o, back_code[:, cols], own_back)
            own_chosen = jnp.where(me == o, all_chosen[:, cols], own_chosen)
        eye = jnp.where(lax.broadcasted_iota(I32, (TOK, TOK), 0) == lax.broadcasted_iota(I32, (TOK, TOK), 1), 1.0, 0.0).astype(BF16)
        bio = lax.broadcasted_iota(I32, (EP * PAIR, TOK), 0)
        tmat[...] = nt(eye, jnp.where(bio == own_back, 1.0, 0.0).astype(BF16)).astype(BF16)
        cio = lax.broadcasted_iota(I32, (EXPERTS, TOK), 0)
        pick = nt(eye, jnp.where(cio == own_chosen, 1.0, 0.0).astype(BF16))
        gcol[...] = jnp.sum(prob * pick, axis=1, keepdims=True)

    def gather(c):
        with scope(f"xwait{c}"):
            csnd[c].wait_recv()
            fwd[c].wait_recv()
        with scope(f"gather{c}"):
            xsr[c][...] = nn(smat, xr[c][...]).astype(BF16)

    steps = [(p, g) for p in range(3) for g in range(NGRP)]
    wts = (wt0, wt1)

    def turn(s, i):
        p, g = steps[s]
        wts[s % 2][i, :KC[p][1], :] = wgr[p][g * GRP + i].T

    def gu_step(s):
        p, g = steps[s]
        n = KC[p][1]
        with scope(f"gu{p}"):
            gu_copy(p, g, 1).wait()
            if s + 1 < len(steps):
                gu_copy(*steps[s + 1], 0).wait()
            for i in range(GRP):
                e = g * GRP + i
                rows = slice(e * SLOT, (e + 1) * SLOT)
                if s + 1 < len(steps):
                    turn(s + 1, i)
                xe = xsr[p][rows, :]
                dg, du = nn(xe, wts[s % 2][i, :n, :]), nt(xe, wur[p][e])
                if p == 0:
                    accg[rows, :] = dg
                    accu[rows, :] = du
                elif p == 1:
                    accg[rows, :] += dg
                    accu[rows, :] += du
                else:
                    hid[rows, :] = silu_mul(accg[rows, :] + dg, accu[rows, :] + du)

    gu_copy(0, 0, 0).wait()
    for i in range(GRP):
        turn(0, i)
    gather(0)
    for s in range(3):
        gu_step(s)
    forward(1)
    gu_step(3)
    start_down(0)
    start_down(4)
    gather(1)
    gu_step(4)
    forward(2)
    for s in range(5, 8):
        gu_step(s)
    start_down(1)
    start_down(2)
    start_down(3)
    gather(2)
    for s in range(8, 12):
        gu_step(s)

    cr, yr = [], []

    def exchange(j):
        with scope(f"cw{j}"):
            for c in cr[j]:
                c.wait_recv()
        ypart[j] = nn(tmat[...], crecv[j]).astype(BF16)
        yr.append(rcopy(ypart.at[j], yrecv.at[j], y_send.at[j], y_recv.at[j], tp=1 - tp))

    my_rows = pl.ds(pl.multiple_of(me * PAIR, PAIR), PAIR)
    for j in range(NCH):
        ref, col = ((w1u, 0), (w2g, 0), (w2g, NC), (w2u, 0), (w1g, 0))[j]

        @pl.loop(0, NGRP)
        def _(g):
            with scope(f"dw{j}"):
                d_copy(j, g).wait()
            for i in range(GRP):
                e = g * GRP + i
                rows = pl.ds(pl.multiple_of(e * SLOT, SLOT), SLOT)
                slot_out[rows, :] = nn(hid[rows, :], ref[e, :, col:col + NC]).astype(BF16)

        with scope(f'gx{j}'):
            csend[j] = nn(gmat[...], slot_out[...]).astype(BF16)
        crecv[j, my_rows, :] = csend[j, my_rows, :]
        row = []
        for d in range(1, EP):
            o = lax.rem(me + d, EP)
            row.append(rcopy(csend.at[j, pl.ds(pl.multiple_of(o * PAIR, PAIR), PAIR)], crecv.at[j, my_rows],
                             c_send.at[j, d - 1], c_recv.at[j, d - 1], ep=o))
        cr.append(row)
        if j >= LAG:
            exchange(j - LAG)

    for j in range(NCH - LAG, NCH):
        exchange(j)
    resc.wait()
    shc.wait_recv()
    oc = []
    for j in range(NCH):
        cols = slice(j * NC, (j + 1) * NC)
        base = res_v[:, cols].astype(F32) + (sh_part[:, cols].astype(F32) + sh_recv[:, cols].astype(F32))
        with scope(f"yw{j}"):
            yr[j].wait_recv()
        routed = (ypart[j].astype(F32) + yrecv[j].astype(F32)).astype(BF16).astype(F32)
        obuf[:, cols] = (base + gcol[...] * routed).astype(BF16)
        oc.append(start(pltpu.make_async_copy(obuf.at[:, pl.ds(j * NC, NC)], out_ref.at[:, pl.ds(j * NC, NC)], o_sem.at[j])))
    with scope('sendwait'):
        for c in sends:
            c.wait_send()
    with scope('outwait'):
        for c in oc:
            c.wait()


def solution(mesh):
    tok_spec, id_spec = P(("dp", "ep"), None), P(("dp", "ep"))

    def device_step(normed, residual, w_router, ws_gate, ws_up, ws_down, we_gate, we_up, we_down, first_id, alt_id):
        hbm = pl.BlockSpec(memory_space=pl.ANY)
        vm, dma = pltpu.VMEM, pltpu.SemaphoreType.DMA
        weights = [vm((LOCAL, FFE, n), BF16) for _, n in KC for _ in range(2)]
        scratch = [vm((ALL, n), BF16) for _, n in KC]
        scratch += [vm((TOK, D), BF16), vm((EXPERTS, D), F32), vm((EP, 1, TOK), I32), vm((EP, 1, TOK), I32)]
        scratch += [vm((D, FFS), BF16), vm((D, FFS), BF16), vm((FFS, D), BF16)] + weights
        scratch += [vm((SLOTS, n), BF16) for _, n in KC]
        scratch += [vm((SLOTS, FFE), F32), vm((SLOTS, FFE), F32), vm((SLOTS, FFE), BF16), vm((TOK, FFS), BF16)]
        scratch += [vm((TOK, D), BF16), vm((TOK, D), BF16), vm((EP * PAIR, SLOTS), BF16), vm((TOK, EP * PAIR), BF16), vm((TOK, 1), F32)]
        scratch += [vm((NCH, EP * PAIR, NC), BF16), vm((NCH, EP * PAIR, NC), BF16), vm((NCH, TOK, NC), BF16), vm((NCH, TOK, NC), BF16), vm((SLOTS, NC), BF16), vm((TOK, D), BF16), vm((GRP, 512, FFE), BF16), vm((GRP, 512, FFE), BF16)]
        scratch += [dma((3,)), dma((2,)), dma((2,)), dma((3,)), dma((3, NGRP, 2)), dma((NCH, NGRP)),
                    dma((3, 3)), dma((3, 3)), dma((2, 3)), dma((2, 3)), dma((2,)), dma((NCH, 3)), dma((NCH, 3)), dma((NCH,)), dma((NCH,)), dma((NCH,))]
        return pl.pallas_call(
            kernel,
            out_shape=jax.ShapeDtypeStruct((TOK, D), BF16),
            in_specs=[hbm] * 11,
            out_specs=hbm,
            scratch_shapes=scratch,
            compiler_params=pltpu.CompilerParams(collective_id=0, has_side_effects=True, vmem_limit_bytes=66_000_000),
            name="moe_layer",
        )(normed, residual, w_router.T, ws_gate, ws_up, ws_down, jnp.swapaxes(we_gate, 1, 2), jnp.swapaxes(we_up, 1, 2), we_down,
          first_id.reshape(1, TOK), alt_id.reshape(1, TOK))

    return jax.shard_map(device_step, mesh=mesh,
                         in_specs=(tok_spec, tok_spec, P(None, None), P(None, "tp"), P(None, "tp"), P("tp", None), P("ep", None, "tp"),
                                   P("ep", None, "tp"), P("ep", "tp", None), id_spec, id_spec),
                         out_specs=tok_spec, check_vma=False)
```

```python
import functools

import jax
import jax.numpy as jnp
from jax import lax
from jax.experimental import pallas as pl
from jax.experimental.pallas import tpu as pltpu
from jax.sharding import PartitionSpec as P

MESH = pl.DeviceIdType.MESH
scope = jax.named_scope
F32, BF16, I32 = jnp.float32, jnp.bfloat16, jnp.int32

EP = 4
TOK = 128
ALL = EP * TOK
EXPERTS = 64
LOCAL = EXPERTS // EP
CAP = 10
SLOT = 16
SLOTS = LOCAL * SLOT
PAIR = 64
D = 1280
FFE = 448
FFS = 896
GRP = 4
NGRP = LOCAL // GRP
KC = ((0, 256), (256, 512), (768, 512))
NC = 256
NCH = D // NC
TPF = (0, 2)
PACK = LOCAL * CAP


def nn(a, b):
    return lax.dot_general(a, b, (((1,), (0,)), ((), ())), preferred_element_type=F32)


def nt(a, b):
    return lax.dot_general(a, b, (((1,), (1,)), ((), ())), preferred_element_type=F32)


def silu_mul(g, u):
    return (g * (1.0 / (1.0 + jnp.exp(-g))) * u).astype(BF16)


def kernel(normed, residual, wr, wsg, wsu, wsd, weg, weu, wed, fid, aid, out_ref,
           x0, x1, x2, res_v, wr_v, fids, aids,
           sg, su, sd, w1g, w1u, w2g, w2u, w3g, w3u,
           xs0, xs1, xs2, accg, accu, hid, hid_s,
           sh_part, sh_recv, gmat, tmat, gcol, csend, crecv, ypart, yrecv, slot_out, wt0, wt1, gpack, pmat,
           l_sem, w_sem, d_sem, snd, r_id, r_x, r_core, r_sh, r_c, r_y):
    me = lax.axis_index("ep")
    tp = lax.axis_index("tp")
    xpeer = lax.rem(me + 2, EP)
    cpeer = me + 1 - 2 * lax.rem(me, 2)
    diag = lax.rem(cpeer + 2, EP)
    xr = (x0, x1, x2)
    xsr = (xs0, xs1, xs2)
    wgr, wur = (w1g, w2g, w3g), (w1u, w2u, w3u)
    mine = pl.ds(pl.multiple_of(me * TOK, TOK), TOK)

    def start(c):
        c.start()
        return c

    def settle(ref, sem):
        pltpu.make_async_copy(ref, ref, sem).wait()

    idc = [start(pltpu.make_async_copy(fid, fids.at[me], l_sem.at[5])),
           start(pltpu.make_async_copy(aid, aids.at[me], l_sem.at[5]))]
    xc = [start(pltpu.make_async_copy(normed.at[:, pl.ds(k, n)], xr[c].at[mine], l_sem.at[0])) for c, (k, n) in enumerate(KC)]
    wrc = start(pltpu.make_async_copy(wr, wr_v, l_sem.at[1]))

    def gu_copy(p, g, i):
        k, n = KC[p]
        src = (weg, weu)[i].at[pl.ds(GRP * g, GRP), :, pl.ds(k, n)]
        return pltpu.make_async_copy(src, (wgr, wur)[i][p].at[pl.ds(GRP * g, GRP)], w_sem.at[p, g])

    def d_buf(j):
        ref, col = ((w1g, 0), (w1u, 0), (w2g, 0), (w2g, NC), (w2u, 0))[j]
        return ref.at[:, :, pl.ds(col, NC)]

    def d_copy(j):
        return pltpu.make_async_copy(wed.at[:, :, pl.ds(j * NC, NC)], d_buf(j), d_sem.at[j])

    def start_pass(p):
        for g in range(NGRP):
            for i in range(2):
                gu_copy(p, g, i).start()


    with scope("barrier"):
        bar = pltpu.get_barrier_semaphore()
        for o in (xpeer, cpeer, diag):
            pl.semaphore_signal(bar, inc=1, device_id={"ep": o}, device_id_type=MESH)
        pl.semaphore_signal(bar, inc=1, device_id={"tp": 1 - tp}, device_id_type=MESH)
        settle(fids.at[pl.ds(0, 2)], l_sem.at[5])
        settle(sh_recv, l_sem.at[0])
        swc = [start(pltpu.make_async_copy(s, d, l_sem.at[(2, 3, 6)[i]])) for i, (s, d) in enumerate(((wsg, sg), (wsu, su), (wsd, sd)))]
        pl.semaphore_wait(bar, 4)

    sends = []

    def rcopy(src, dst, r, s, **dev):
        c = pltpu.make_async_remote_copy(src_ref=src, dst_ref=dst, send_sem=snd.at[s], recv_sem=r, device_id=dev, device_id_type=MESH)
        c.start()
        sends.append(c)
        return c

    idr = []
    for d in range(1, EP):
        o = lax.rem(me + d, EP)
        for i, ref in enumerate((fids, aids)):
            idr.append(rcopy(ref.at[me], ref.at[me], r_id.at[i], 2 + i, ep=o))
    with scope("xsend"):
        xsend, csnd, fwd = [], [], []
        for c in range(3):
            xsend.append(rcopy(xr[c].at[mine], xr[c].at[mine], r_x.at[c], 0, ep=xpeer))
        for c in range(3):
            csnd.append(rcopy(xr[c].at[mine], xr[c].at[mine], r_core.at[c], 0, ep=cpeer))

    theirs = pl.ds(pl.multiple_of(xpeer * TOK, TOK), TOK)

    def forward(c):
        with scope(f"fwait{c}"):
            xsend[c].wait_recv()
        fwd.append(rcopy(xr[c].at[theirs], xr[c].at[theirs], r_core.at[c], 0, ep=cpeer))

    xo = [xr[c][mine, :] for c in range(3)]
    with scope("shwait"):
        swc[0].wait()
        swc[1].wait()
    start_pass(0)
    resc = start(pltpu.make_async_copy(residual, res_v, l_sem.at[4]))
    with scope("shgu"):
        for n0 in range(0, FFS, 256):
            n = min(256, FFS - n0)
            g = sum(nn(xr[c][mine, :], sg[k:k + kn, n0:n0 + n]) for c, (k, kn) in enumerate(KC))
            u = sum(nn(xr[c][mine, :], su[k:k + kn, n0:n0 + n]) for c, (k, kn) in enumerate(KC))
            hid_s[:, n0:n0 + n] = silu_mul(g, u)
    with scope("shdown"):
        swc[2].wait()
        for n0 in range(0, D, 256):
            sh_part[:, n0:n0 + 256] = nn(hid_s[...], sd[:, n0:n0 + 256]).astype(BF16)
    start_pass(1)
    start_pass(2)

    forward(0)
    with scope("router"):
        wrc.wait()
        wr_hi = wr_v[...].astype(BF16)
        wr_lo = (wr_v[...] - wr_hi.astype(F32)).astype(BF16)
        logits = jnp.zeros((TOK, EXPERTS), F32)
        for c, (k, kn) in enumerate(KC):
            logits = logits + nt(xo[c], wr_hi[:, k:k + kn]) + nt(xo[c], wr_lo[:, k:k + kn])
        ex = jnp.exp(logits - jnp.max(logits, axis=1, keepdims=True))
        prob = ex / jnp.sum(ex, axis=1, keepdims=True)
    shc = rcopy(sh_part, sh_recv, r_sh.at[0], 0, tp=1 - tp)

    with scope("idwait"):
        settle(fids.at[pl.ds(0, EP - 1)], r_id.at[0])
        settle(aids.at[pl.ds(0, EP - 1)], r_id.at[1])
    with scope("routing"):
        f = jnp.concatenate([fids[o] for o in range(EP)], axis=1)
        a = jnp.concatenate([aids[o] for o in range(EP)], axis=1)
        ti, tj = lax.broadcasted_iota(I32, (ALL, ALL), 0), lax.broadcasted_iota(I32, (ALL, ALL), 1)
        before = jnp.where(ti < tj, 1.0, 0.0)
        before_dev = jnp.where((ti // TOK) == (tj // TOK), before, 0.0).astype(BF16)
        before = before.astype(BF16)
        eio = lax.broadcasted_iota(I32, (EXPERTS, ALL), 0)
        one_f = jnp.where(eio == f, 1.0, 0.0)
        one_a = jnp.where(eio == a, 1.0, 0.0)
        rank_f = jnp.sum(nn(one_f.astype(BF16), before) * one_f, axis=0, keepdims=True)
        kept = rank_f < CAP - 0.5
        load = jnp.minimum(jnp.sum(one_f, axis=1, keepdims=True), float(CAP))
        over_a = one_a * jnp.where(kept, 0.0, 1.0)
        rank_a = jnp.sum(nn(over_a.astype(BF16), before) * over_a, axis=0, keepdims=True)
        load_a = jnp.sum(one_a * load, axis=0, keepdims=True)
        active = kept | (rank_a + load_a < CAP - 0.5)
        chosen = jnp.where(kept, f, a)
        slot = jnp.where(kept, rank_f, load_a + rank_a).astype(I32)
        owner = chosen // LOCAL
        local = chosen - owner * LOCAL
        here = active & (owner == me)
        slot_code = jnp.where(here, local * SLOT + slot, -1)
        oio = lax.broadcasted_iota(I32, (16, ALL), 0)
        own_f = jnp.where(oio == f // LOCAL, 1.0, 0.0)
        own_a = jnp.where(oio == a // LOCAL + EP, 1.0, 0.0)
        seen = nn((own_f + own_a).astype(BF16), before_dev)
        pos_f = jnp.sum(seen * own_f, axis=0, keepdims=True)
        pos_a = jnp.sum(seen * own_a, axis=0, keepdims=True)
        pos = jnp.where(kept, pos_f, pos_a + PAIR // 2).astype(I32)
        origin = lax.broadcasted_iota(I32, (1, ALL), 1) // TOK
        pair_code = jnp.where(here, origin * PAIR + pos, -1)
        back_code = jnp.where(active, owner * PAIR + pos, -1)
        sio = lax.broadcasted_iota(I32, (SLOTS, ALL), 0)
        smat = jnp.where(sio == slot_code, 1.0, 0.0).astype(BF16)
        rmat = jnp.where(sio == pair_code, 1.0, 0.0).astype(BF16)
        gmat[...] = nt(rmat, smat).astype(BF16)
        pio = lax.broadcasted_iota(I32, (PACK, ALL), 0)
        gpack[...] = nt(rmat, jnp.where(pio == jnp.where(here, local * CAP + slot, -1), 1.0, 0.0).astype(BF16)).astype(BF16)
        col = lax.broadcasted_iota(I32, (PACK, SLOTS), 1)
        packed_row = jnp.where(col % SLOT < CAP, (col // SLOT) * CAP + col % SLOT, -1)
        pmat[...] = jnp.where(lax.broadcasted_iota(I32, (PACK, SLOTS), 0) == packed_row, 1.0, 0.0).astype(BF16)

        own_back, own_chosen = back_code[:, :TOK], jnp.where(active, chosen, -1)[:, :TOK]
        all_chosen = jnp.where(active, chosen, -1)
        for o in range(1, EP):
            cols = slice(o * TOK, (o + 1) * TOK)
            own_back = jnp.where(me == o, back_code[:, cols], own_back)
            own_chosen = jnp.where(me == o, all_chosen[:, cols], own_chosen)
        eye = jnp.where(lax.broadcasted_iota(I32, (TOK, TOK), 0) == lax.broadcasted_iota(I32, (TOK, TOK), 1), 1.0, 0.0).astype(BF16)
        bio = lax.broadcasted_iota(I32, (EP * PAIR, TOK), 0)
        tmat[...] = nt(eye, jnp.where(bio == own_back, 1.0, 0.0).astype(BF16)).astype(BF16)
        cio = lax.broadcasted_iota(I32, (EXPERTS, TOK), 0)
        pick = nt(eye, jnp.where(cio == own_chosen, 1.0, 0.0).astype(BF16))
        gcol[...] = jnp.sum(prob * pick, axis=1, keepdims=True)

    def gather(c):
        with scope(f"xwait{c}"):
            settle(xr[c].at[pl.ds(0, 2 * TOK)], r_core.at[c])
        with scope(f"gather{c}"):
            xsr[c][...] = nn(smat, xr[c][...]).astype(BF16)

    steps = [(p, g) for p in range(3) for g in range(NGRP)]
    wts = (wt0, wt1)

    def arrived(s):
        p, g = steps[s]
        settle(wgr[p].at[pl.ds(0, 2 * GRP)], w_sem.at[p, g])

    def turn(s, i):
        p, g = steps[s]
        wts[s % 2][i, :KC[p][1], :] = wgr[p][g * GRP + i].T

    def gu_step(s):
        p, g = steps[s]
        n = KC[p][1]
        with scope(f"gu{p}"):
            if s + 1 < len(steps):
                arrived(s + 1)
            for i in range(GRP):
                e = g * GRP + i
                rows = slice(e * SLOT, (e + 1) * SLOT)
                if s + 1 < len(steps):
                    turn(s + 1, i)
                xe = xsr[p][rows, :]
                dg, du = nn(xe, wts[s % 2][i, :n, :]), nt(xe, wur[p][e])
                if p == 0:
                    accg[rows, :] = dg
                    accu[rows, :] = du
                elif p == 1:
                    accg[rows, :] += dg
                    accu[rows, :] += du
                else:
                    hid[rows, :] = silu_mul(accg[rows, :] + dg, accu[rows, :] + du)

    arrived(0)
    for i in range(GRP):
        turn(0, i)
    gather(0)
    for s in range(3):
        gu_step(s)
    forward(1)
    gu_step(3)
    d_copy(0).start()
    d_copy(1).start()
    gather(1)
    gu_step(4)
    forward(2)
    for s in range(5, 8):
        gu_step(s)
    d_copy(2).start()
    d_copy(3).start()
    d_copy(4).start()
    gather(2)
    for s in range(8, 12):
        gu_step(s)

    my_rows = pl.ds(pl.multiple_of(me * PAIR, PAIR), PAIR)

    def go_back(j, rows):
        csend[j] = rows.astype(BF16)
        crecv[j, my_rows, :] = csend[j, my_rows, :]
        out = []
        for d in range(1, EP):
            o = lax.rem(me + d, EP)
            out.append(rcopy(csend.at[j, pl.ds(pl.multiple_of(o * PAIR, PAIR), PAIR)], crecv.at[j, my_rows], r_c.at[j], 1, ep=o))
        return out

    back, over = {}, {}
    for j in range(NCH):
        with scope(f"dw{j}"):
            d_copy(j).wait()
        with scope(f"dn{j}"):
            so, wd = slot_out.at[j % 2], d_buf(j)
            for e in range(LOCAL):
                rows = slice(e * SLOT, (e + 1) * SLOT)
                so[rows, :] = nn(hid[rows, :], wd[e]).astype(BF16)
            if j in TPF:
                ypart[j, :PACK, :] = nn(pmat[...], so[...]).astype(BF16)
                over[j] = rcopy(ypart.at[j, pl.ds(0, PACK)], yrecv.at[j, pl.ds(0, PACK)], r_y.at[j], 1, tp=1 - tp)
            else:
                back[j] = go_back(j, nn(gmat[...], so[...]))

    def first_leg(j):
        if j in TPF:
            with scope(f"fy{j}"):
                over[j].wait_recv()
            r = (ypart[j, :PACK, :].astype(F32) + yrecv[j, :PACK, :].astype(F32)).astype(BF16)
            back[j] = go_back(j, nn(gpack[...], r))
        else:
            with scope(f"fx{j}"):
                settle(crecv.at[j, pl.ds(0, (EP - 1) * PAIR)], r_c.at[j])
            ypart[j, :TOK, :] = nn(tmat[...], crecv[j]).astype(BF16)
            over[j] = rcopy(ypart.at[j, pl.ds(0, TOK)], yrecv.at[j, pl.ds(0, TOK)], r_y.at[j], 1, tp=1 - tp)

    for j in (0, 1, 2, 3, 4):
        first_leg(j)
    with scope("shrecv"):
        resc.wait()
        shc.wait_recv()
    for j in (1, 0, 3, 2, 4):
        cols = slice(j * NC, (j + 1) * NC)
        base = res_v[:, cols].astype(F32) + (sh_part[:, cols].astype(F32) + sh_recv[:, cols].astype(F32))
        with scope(f"last{j}"):
            if j in TPF:
                settle(crecv.at[j, pl.ds(0, (EP - 1) * PAIR)], r_c.at[j])
            else:
                over[j].wait_recv()
        if j in TPF:
            routed = nn(tmat[...], crecv[j])
        else:
            routed = (ypart[j, :TOK, :].astype(F32) + yrecv[j, :TOK, :].astype(F32)).astype(BF16).astype(F32)
        out_ref[:, cols] = (base + gcol[...] * routed).astype(BF16)
    with scope('sendwait'):
        settle(sd.at[pl.ds(0, 4 * TOK)], snd.at[0])
        back_rows = NCH * (EP - 1) * PAIR + len(TPF) * PACK + (NCH - len(TPF)) * TOK
        settle(sd.at[pl.ds(0, back_rows // 2), pl.ds(0, 2 * NC)], snd.at[1])
        settle(fids.at[pl.ds(0, EP - 1)], snd.at[2])
        settle(aids.at[pl.ds(0, EP - 1)], snd.at[3])


def solution(mesh):
    tok_spec, id_spec = P(("dp", "ep"), None), P(("dp", "ep"))

    def device_step(normed, residual, w_router, ws_gate, ws_up, ws_down, we_gate, we_up, we_down, first_id, alt_id):
        hbm = pl.BlockSpec(memory_space=pl.ANY)
        vm, dma = pltpu.VMEM, pltpu.SemaphoreType.DMA
        weights = [vm((LOCAL, FFE, n), BF16) for _, n in KC for _ in range(2)]
        scratch = [vm((ALL, n), BF16) for _, n in KC]
        scratch += [vm((TOK, D), BF16), vm((EXPERTS, D), F32), vm((EP, 1, TOK), I32), vm((EP, 1, TOK), I32)]
        scratch += [vm((D, FFS), BF16), vm((D, FFS), BF16), vm((FFS, D), BF16)] + weights
        scratch += [vm((SLOTS, n), BF16) for _, n in KC]
        scratch += [vm((SLOTS, FFE), F32), vm((SLOTS, FFE), F32), vm((SLOTS, FFE), BF16), vm((TOK, FFS), BF16)]
        scratch += [vm((TOK, D), BF16), vm((TOK, D), BF16), vm((EP * PAIR, SLOTS), BF16), vm((TOK, EP * PAIR), BF16), vm((TOK, 1), F32)]
        scratch += [vm((NCH, EP * PAIR, NC), BF16), vm((NCH, EP * PAIR, NC), BF16), vm((NCH, PACK, NC), BF16), vm((NCH, PACK, NC), BF16), vm((2, SLOTS, NC), BF16), vm((GRP, 512, FFE), BF16), vm((GRP, 512, FFE), BF16), vm((EP * PAIR, PACK), BF16), vm((PACK, SLOTS), BF16)]
        scratch += [dma((7,)), dma((3, NGRP)), dma((NCH,)), dma((4,)), dma((2,)), dma((3,)), dma((3,)), dma((1,)), dma((NCH,)), dma((NCH,))]
        return pl.pallas_call(
            kernel,
            out_shape=pltpu.VMEM((TOK, D), BF16),
            in_specs=[hbm] * 11,
            out_specs=pl.BlockSpec(memory_space=pltpu.VMEM),
            scratch_shapes=scratch,
            compiler_params=pltpu.CompilerParams(collective_id=0, has_side_effects=True, vmem_limit_bytes=62_000_000),
            name="moe_layer",
        )(normed, residual, w_router.T, ws_gate, ws_up, ws_down, jnp.swapaxes(we_gate, 1, 2), jnp.swapaxes(we_up, 1, 2), we_down,
          first_id.reshape(1, TOK), alt_id.reshape(1, TOK))

    return jax.shard_map(device_step, mesh=mesh,
                         in_specs=(tok_spec, tok_spec, P(None, None), P(None, "tp"), P(None, "tp"), P("tp", None), P("ep", None, "tp"),
                                   P("ep", None, "tp"), P("ep", "tp", None), id_spec, id_spec),
                         out_specs=tok_spec, check_vma=False)
```

```python
import functools

import jax
import jax.numpy as jnp
from jax import lax
from jax.experimental import pallas as pl
from jax.experimental.pallas import tpu as pltpu
from jax.sharding import PartitionSpec as P

MESH = pl.DeviceIdType.MESH
scope = jax.named_scope
F32, BF16, I32 = jnp.float32, jnp.bfloat16, jnp.int32

EP = 4
TOK = 128
ALL = EP * TOK
EXPERTS = 64
LOCAL = EXPERTS // EP
CAP = 10
SLOT = 16
SLOTS = LOCAL * SLOT
PAIR = 64
D = 1280
FFE = 448
FFS = 896
GRP = 4
NGRP = LOCAL // GRP
KC = ((0, 256), (256, 256), (512, 256), (768, 512))
NC = 256
NCH = D // NC
TPF = (1, 3)
PACK = LOCAL * CAP


def nn(a, b):
    return lax.dot_general(a, b, (((1,), (0,)), ((), ())), preferred_element_type=F32)


def nt(a, b):
    return lax.dot_general(a, b, (((1,), (1,)), ((), ())), preferred_element_type=F32)


def silu_mul(g, u):
    return (g * (1.0 / (1.0 + jnp.exp(-g))) * u).astype(BF16)


def kernel(normed, residual, wr, wsg, wsu, wsd, weg, weu, wed, fid, aid, out_ref,
           x0, x1, x2, x3, res_v, wr_v, fids, aids,
           sg, su, sd, w1g, w1u, w2g, w2u, w3g, w3u, w4g, w4u,
           xs0, xs1, xs2, xs3, accg, accu, hid, hid_s,
           sh_part, sh_recv, gmat, tmat, gcol, csend, crecv, ypart, yrecv, slot_out, wt0, wt1, gpack, pmat,
           l_sem, w_sem, d_sem, snd, r_id, r_x, r_core, r_sh, r_c, r_y):
    me = lax.axis_index("ep")
    tp = lax.axis_index("tp")
    xpeer = lax.rem(me + 2, EP)
    cpeer = me + 1 - 2 * lax.rem(me, 2)
    diag = lax.rem(cpeer + 2, EP)
    xr = (x0, x1, x2, x3)
    xsr = (xs0, xs1, xs2, xs3)
    wgr, wur = (w1g, w2g, w3g, w4g), (w1u, w2u, w3u, w4u)
    mine = pl.ds(pl.multiple_of(me * TOK, TOK), TOK)

    def start(c):
        c.start()
        return c

    def settle(ref, sem):
        pltpu.make_async_copy(ref, ref, sem).wait()

    idc = [start(pltpu.make_async_copy(fid, fids.at[me], l_sem.at[5])),
           start(pltpu.make_async_copy(aid, aids.at[me], l_sem.at[5]))]
    xc = [start(pltpu.make_async_copy(normed.at[:, pl.ds(k, n)], xr[c].at[mine], l_sem.at[0])) for c, (k, n) in enumerate(KC)]
    wrc = start(pltpu.make_async_copy(wr, wr_v, l_sem.at[1]))

    def gu_copy(p, g, i):
        k, n = KC[p]
        src = (weg, weu)[i].at[pl.ds(GRP * g, GRP), :, pl.ds(k, n)]
        return pltpu.make_async_copy(src, (wgr, wur)[i][p].at[pl.ds(GRP * g, GRP)], w_sem.at[p, g])

    def d_buf(j):
        return (w1g, w1u, w2g, w2u, w3g)[j]

    def d_copy(j):
        return pltpu.make_async_copy(wed.at[:, :, pl.ds(j * NC, NC)], d_buf(j), d_sem.at[j])

    def start_pass(p):
        for g in range(NGRP):
            for i in range(2):
                gu_copy(p, g, i).start()


    with scope("barrier"):
        bar = pltpu.get_barrier_semaphore()
        for o in (xpeer, cpeer, diag):
            pl.semaphore_signal(bar, inc=1, device_id={"ep": o}, device_id_type=MESH)
        pl.semaphore_signal(bar, inc=1, device_id={"tp": 1 - tp}, device_id_type=MESH)
        settle(fids.at[pl.ds(0, 2)], l_sem.at[5])
        settle(sh_recv, l_sem.at[0])
        swc = [start(pltpu.make_async_copy(s, d, l_sem.at[(2, 3, 6)[i]])) for i, (s, d) in enumerate(((wsg, sg), (wsu, su), (wsd, sd)))]
        pl.semaphore_wait(bar, 4)

    sends = []

    def rcopy(src, dst, r, s, **dev):
        c = pltpu.make_async_remote_copy(src_ref=src, dst_ref=dst, send_sem=snd.at[s], recv_sem=r, device_id=dev, device_id_type=MESH)
        c.start()
        sends.append(c)
        return c

    idr = []
    for d in range(1, EP):
        o = lax.rem(me + d, EP)
        for i, ref in enumerate((fids, aids)):
            idr.append(rcopy(ref.at[me], ref.at[me], r_id.at[i], 2 + i, ep=o))
    with scope("xsend"):
        xsend, csnd, fwd = [], [], []
        for c in range(len(KC)):
            xsend.append(rcopy(xr[c].at[mine], xr[c].at[mine], r_x.at[c], 0, ep=xpeer))
        for c in range(len(KC)):
            csnd.append(rcopy(xr[c].at[mine], xr[c].at[mine], r_core.at[c], 0, ep=cpeer))

    theirs = pl.ds(pl.multiple_of(xpeer * TOK, TOK), TOK)

    def forward(c):
        with scope(f"fwait{c}"):
            xsend[c].wait_recv()
        fwd.append(rcopy(xr[c].at[theirs], xr[c].at[theirs], r_core.at[c], 0, ep=cpeer))

    xo = [xr[c][mine, :] for c in range(len(KC))]
    with scope("router"):
        wrc.wait()
        wr_hi = wr_v[...].astype(BF16)
        wr_lo = (wr_v[...] - wr_hi.astype(F32)).astype(BF16)
        logits = jnp.zeros((TOK, EXPERTS), F32)
        for c, (k, kn) in enumerate(KC):
            logits = logits + nt(xo[c], wr_hi[:, k:k + kn]) + nt(xo[c], wr_lo[:, k:k + kn])
        ex = jnp.exp(logits - jnp.max(logits, axis=1, keepdims=True))
        prob = ex / jnp.sum(ex, axis=1, keepdims=True)
    with scope("shwait"):
        swc[0].wait()
        swc[1].wait()
    start_pass(0)
    resc = start(pltpu.make_async_copy(residual, res_v, l_sem.at[4]))
    with scope("shgu"):
        for n0 in range(0, FFS, 256):
            n = min(256, FFS - n0)
            g = sum(nn(xr[c][mine, :], sg[k:k + kn, n0:n0 + n]) for c, (k, kn) in enumerate(KC))
            u = sum(nn(xr[c][mine, :], su[k:k + kn, n0:n0 + n]) for c, (k, kn) in enumerate(KC))
            hid_s[:, n0:n0 + n] = silu_mul(g, u)
    with scope("shdown"):
        swc[2].wait()
        for n0 in range(0, D, 256):
            sh_part[:, n0:n0 + 256] = nn(hid_s[...], sd[:, n0:n0 + 256]).astype(BF16)
    start_pass(1)
    start_pass(2)
    start_pass(3)

    forward(0)
    shc = rcopy(sh_part, sh_recv, r_sh.at[0], 0, tp=1 - tp)

    with scope("idwait"):
        settle(fids.at[pl.ds(0, EP - 1)], r_id.at[0])
        settle(aids.at[pl.ds(0, EP - 1)], r_id.at[1])
    with scope("routing"):
        f = jnp.concatenate([fids[o] for o in range(EP)], axis=1)
        a = jnp.concatenate([aids[o] for o in range(EP)], axis=1)
        ti, tj = lax.broadcasted_iota(I32, (ALL, ALL), 0), lax.broadcasted_iota(I32, (ALL, ALL), 1)
        before = jnp.where(ti < tj, 1.0, 0.0)
        before_dev = jnp.where((ti // TOK) == (tj // TOK), before, 0.0).astype(BF16)
        before = before.astype(BF16)
        eio = lax.broadcasted_iota(I32, (EXPERTS, ALL), 0)
        one_f = jnp.where(eio == f, 1.0, 0.0)
        one_a = jnp.where(eio == a, 1.0, 0.0)
        rank_f = jnp.sum(nn(one_f.astype(BF16), before) * one_f, axis=0, keepdims=True)
        kept = rank_f < CAP - 0.5
        load = jnp.minimum(jnp.sum(one_f, axis=1, keepdims=True), float(CAP))
        over_a = one_a * jnp.where(kept, 0.0, 1.0)
        rank_a = jnp.sum(nn(over_a.astype(BF16), before) * over_a, axis=0, keepdims=True)
        load_a = jnp.sum(one_a * load, axis=0, keepdims=True)
        active = kept | (rank_a + load_a < CAP - 0.5)
        chosen = jnp.where(kept, f, a)
        slot = jnp.where(kept, rank_f, load_a + rank_a).astype(I32)
        owner = chosen // LOCAL
        local = chosen - owner * LOCAL
        here = active & (owner == me)
        slot_code = jnp.where(here, local * SLOT + slot, -1)
        oio = lax.broadcasted_iota(I32, (16, ALL), 0)
        own_f = jnp.where(oio == f // LOCAL, 1.0, 0.0)
        own_a = jnp.where(oio == a // LOCAL + EP, 1.0, 0.0)
        seen = nn((own_f + own_a).astype(BF16), before_dev)
        pos_f = jnp.sum(seen * own_f, axis=0, keepdims=True)
        pos_a = jnp.sum(seen * own_a, axis=0, keepdims=True)
        pos = jnp.where(kept, pos_f, pos_a + PAIR // 2).astype(I32)
        origin = lax.broadcasted_iota(I32, (1, ALL), 1) // TOK
        pair_code = jnp.where(here, origin * PAIR + pos, -1)
        back_code = jnp.where(active, owner * PAIR + pos, -1)
        sio = lax.broadcasted_iota(I32, (SLOTS, ALL), 0)
        smat = jnp.where(sio == slot_code, 1.0, 0.0).astype(BF16)
        rmat = jnp.where(sio == pair_code, 1.0, 0.0).astype(BF16)
        gmat[...] = nt(rmat, smat).astype(BF16)
        pio = lax.broadcasted_iota(I32, (PACK, ALL), 0)
        gpack[...] = nt(rmat, jnp.where(pio == jnp.where(here, local * CAP + slot, -1), 1.0, 0.0).astype(BF16)).astype(BF16)
        col = lax.broadcasted_iota(I32, (PACK, SLOTS), 1)
        packed_row = jnp.where(col % SLOT < CAP, (col // SLOT) * CAP + col % SLOT, -1)
        pmat[...] = jnp.where(lax.broadcasted_iota(I32, (PACK, SLOTS), 0) == packed_row, 1.0, 0.0).astype(BF16)

        own_back, own_chosen = back_code[:, :TOK], jnp.where(active, chosen, -1)[:, :TOK]
        all_chosen = jnp.where(active, chosen, -1)
        for o in range(1, EP):
            cols = slice(o * TOK, (o + 1) * TOK)
            own_back = jnp.where(me == o, back_code[:, cols], own_back)
            own_chosen = jnp.where(me == o, all_chosen[:, cols], own_chosen)
        eye = jnp.where(lax.broadcasted_iota(I32, (TOK, TOK), 0) == lax.broadcasted_iota(I32, (TOK, TOK), 1), 1.0, 0.0).astype(BF16)
        bio = lax.broadcasted_iota(I32, (EP * PAIR, TOK), 0)
        tmat[...] = nt(eye, jnp.where(bio == own_back, 1.0, 0.0).astype(BF16)).astype(BF16)
        cio = lax.broadcasted_iota(I32, (EXPERTS, TOK), 0)
        pick = nt(eye, jnp.where(cio == own_chosen, 1.0, 0.0).astype(BF16))
        gcol[...] = jnp.sum(prob * pick, axis=1, keepdims=True)

    def gather(c):
        with scope(f"xwait{c}"):
            settle(xr[c].at[pl.ds(0, 2 * TOK)], r_core.at[c])
        with scope(f"gather{c}"):
            xsr[c][...] = nn(smat, xr[c][...]).astype(BF16)

    steps = [(p, g) for p in range(len(KC)) for g in range(NGRP)]
    wts = (wt0, wt1)

    def arrived(s):
        p, g = steps[s]
        settle(wgr[p].at[pl.ds(0, 2 * GRP)], w_sem.at[p, g])

    def turn(s, i):
        p, g = steps[s]
        wts[s % 2][i, :KC[p][1], :] = wgr[p][g * GRP + i].T

    def gu_step(s):
        p, g = steps[s]
        n = KC[p][1]
        with scope(f"gu{p}"):
            if s + 1 < len(steps):
                arrived(s + 1)
            for i in range(GRP):
                e = g * GRP + i
                rows = slice(e * SLOT, (e + 1) * SLOT)
                if s + 1 < len(steps):
                    turn(s + 1, i)
                xe = xsr[p][rows, :]
                dg, du = nn(xe, wts[s % 2][i, :n, :]), nt(xe, wur[p][e])
                if p == 0:
                    accg[rows, :] = dg
                    accu[rows, :] = du
                elif p < len(KC) - 1:
                    accg[rows, :] += dg
                    accu[rows, :] += du
                else:
                    hid[rows, :] = silu_mul(accg[rows, :] + dg, accu[rows, :] + du)

    arrived(0)
    for i in range(GRP):
        turn(0, i)
    gather(0)
    gu_step(0)
    gu_step(1)
    forward(1)
    gu_step(2)
    gu_step(3)
    d_copy(0).start()
    d_copy(1).start()
    gather(1)
    gu_step(4)
    forward(2)
    gu_step(5)
    gu_step(6)
    gu_step(7)
    d_copy(2).start()
    d_copy(3).start()
    gather(2)
    gu_step(8)
    forward(3)
    gu_step(9)
    gu_step(10)
    gu_step(11)
    d_copy(4).start()
    gather(3)
    for s in range(12, 16):
        gu_step(s)

    my_rows = pl.ds(pl.multiple_of(me * PAIR, PAIR), PAIR)

    def go_back(j, rows):
        csend[j] = rows.astype(BF16)
        crecv[j, my_rows, :] = csend[j, my_rows, :]
        out = []
        for d in range(1, EP):
            o = lax.rem(me + d, EP)
            out.append(rcopy(csend.at[j, pl.ds(pl.multiple_of(o * PAIR, PAIR), PAIR)], crecv.at[j, my_rows], r_c.at[j], 1, ep=o))
        return out

    back, over = {}, {}
    for j in range(NCH):
        with scope(f"dw{j}"):
            d_copy(j).wait()
        with scope(f"dn{j}"):
            so, wd = slot_out.at[j % 2], d_buf(j)
            for e in range(LOCAL):
                rows = slice(e * SLOT, (e + 1) * SLOT)
                so[rows, :] = nn(hid[rows, :], wd[e]).astype(BF16)
            if j in TPF:
                ypart[j, :PACK, :] = nn(pmat[...], so[...]).astype(BF16)
                over[j] = rcopy(ypart.at[j, pl.ds(0, PACK)], yrecv.at[j, pl.ds(0, PACK)], r_y.at[j], 1, tp=1 - tp)
            else:
                back[j] = go_back(j, nn(gmat[...], so[...]))

    def first_leg(j):
        if j in TPF:
            with scope(f"fy{j}"):
                over[j].wait_recv()
            r = (ypart[j, :PACK, :].astype(F32) + yrecv[j, :PACK, :].astype(F32)).astype(BF16)
            back[j] = go_back(j, nn(gpack[...], r))
        else:
            with scope(f"fx{j}"):
                settle(crecv.at[j, pl.ds(0, (EP - 1) * PAIR)], r_c.at[j])
            ypart[j, :TOK, :] = nn(tmat[...], crecv[j]).astype(BF16)
            over[j] = rcopy(ypart.at[j, pl.ds(0, TOK)], yrecv.at[j, pl.ds(0, TOK)], r_y.at[j], 1, tp=1 - tp)

    for j in (0, 1, 2, 3, 4):
        first_leg(j)
    with scope("shrecv"):
        resc.wait()
        shc.wait_recv()
    for j in (0, 1, 2, 3, 4):
        cols = slice(j * NC, (j + 1) * NC)
        base = res_v[:, cols].astype(F32) + (sh_part[:, cols].astype(F32) + sh_recv[:, cols].astype(F32))
        with scope(f"last{j}"):
            if j in TPF:
                settle(crecv.at[j, pl.ds(0, (EP - 1) * PAIR)], r_c.at[j])
            else:
                over[j].wait_recv()
        if j in TPF:
            routed = nn(tmat[...], crecv[j])
        else:
            routed = (ypart[j, :TOK, :].astype(F32) + yrecv[j, :TOK, :].astype(F32)).astype(BF16).astype(F32)
        out_ref[:, cols] = (base + gcol[...] * routed).astype(BF16)
    with scope('sendwait'):
        settle(sd.at[pl.ds(0, 4 * TOK)], snd.at[0])
        back_rows = NCH * (EP - 1) * PAIR + len(TPF) * PACK + (NCH - len(TPF)) * TOK
        settle(sd.at[pl.ds(0, back_rows // 2), pl.ds(0, 2 * NC)], snd.at[1])
        settle(fids.at[pl.ds(0, EP - 1)], snd.at[2])
        settle(aids.at[pl.ds(0, EP - 1)], snd.at[3])


def solution(mesh):
    tok_spec, id_spec = P(("dp", "ep"), None), P(("dp", "ep"))

    def device_step(normed, residual, w_router, ws_gate, ws_up, ws_down, we_gate, we_up, we_down, first_id, alt_id):
        hbm = pl.BlockSpec(memory_space=pl.ANY)
        vm, dma = pltpu.VMEM, pltpu.SemaphoreType.DMA
        weights = [vm((LOCAL, FFE, n), BF16) for _, n in KC for _ in range(2)]
        scratch = [vm((ALL, n), BF16) for _, n in KC]
        scratch += [vm((TOK, D), BF16), vm((EXPERTS, D), F32), vm((EP, 1, TOK), I32), vm((EP, 1, TOK), I32)]
        scratch += [vm((D, FFS), BF16), vm((D, FFS), BF16), vm((FFS, D), BF16)] + weights
        scratch += [vm((SLOTS, n), BF16) for _, n in KC]
        scratch += [vm((SLOTS, FFE), F32), vm((SLOTS, FFE), F32), vm((SLOTS, FFE), BF16), vm((TOK, FFS), BF16)]
        scratch += [vm((TOK, D), BF16), vm((TOK, D), BF16), vm((EP * PAIR, SLOTS), BF16), vm((TOK, EP * PAIR), BF16), vm((TOK, 1), F32)]
        scratch += [vm((NCH, EP * PAIR, NC), BF16), vm((NCH, EP * PAIR, NC), BF16), vm((NCH, PACK, NC), BF16), vm((NCH, PACK, NC), BF16), vm((2, SLOTS, NC), BF16), vm((GRP, 512, FFE), BF16), vm((GRP, 512, FFE), BF16), vm((EP * PAIR, PACK), BF16), vm((PACK, SLOTS), BF16)]
        scratch += [dma((7,)), dma((len(KC), NGRP)), dma((NCH,)), dma((4,)), dma((2,)), dma((len(KC),)), dma((len(KC),)), dma((1,)), dma((NCH,)), dma((NCH,))]
        return pl.pallas_call(
            kernel,
            out_shape=pltpu.VMEM((TOK, D), BF16),
            in_specs=[hbm] * 11,
            out_specs=pl.BlockSpec(memory_space=pltpu.VMEM),
            scratch_shapes=scratch,
            compiler_params=pltpu.CompilerParams(collective_id=0, has_side_effects=True, vmem_limit_bytes=62_000_000),
            name="moe_layer",
        )(normed, residual, w_router.T, ws_gate, ws_up, ws_down, jnp.swapaxes(we_gate, 1, 2), jnp.swapaxes(we_up, 1, 2), we_down,
          first_id.reshape(1, TOK), alt_id.reshape(1, TOK))

    return jax.shard_map(device_step, mesh=mesh,
                         in_specs=(tok_spec, tok_spec, P(None, None), P(None, "tp"), P(None, "tp"), P("tp", None), P("ep", None, "tp"),
                                   P("ep", None, "tp"), P("ep", "tp", None), id_spec, id_spec),
                         out_specs=tok_spec, check_vma=False)
```

```python
import functools

import jax
import jax.numpy as jnp
from jax import lax
from jax.experimental import pallas as pl
from jax.experimental.pallas import tpu as pltpu
from jax.sharding import PartitionSpec as P

MESH = pl.DeviceIdType.MESH
scope = jax.named_scope
F32, BF16, I32 = jnp.float32, jnp.bfloat16, jnp.int32

EP = 4
TOK = 128
ALL = EP * TOK
EXPERTS = 64
LOCAL = EXPERTS // EP
CAP = 10
SLOT = 16
SLOTS = LOCAL * SLOT
PAIR = 64
D = 1280
FFE = 448
FFS = 896
GRP = 4
NGRP = LOCAL // GRP
DIRECT = 1
KC = ((0, 256), (256, 256), (512, 768))
NC = 256
NCH = D // NC
TPF = (1, 3)
PACK = LOCAL * CAP


def nn(a, b):
    return lax.dot_general(a, b, (((1,), (0,)), ((), ())), preferred_element_type=F32)


def nt(a, b):
    return lax.dot_general(a, b, (((1,), (1,)), ((), ())), preferred_element_type=F32)


def silu_mul(g, u):
    return (g * (1.0 / (1.0 + jnp.exp(-g))) * u).astype(BF16)


def kernel(normed, residual, wr, wsg, wsu, wsd, weg, weu, wed, fid, aid, out_ref,
           x0, x1, x2, res_v, wr_v, ids,
           sg, su, sd, w1g, w1u, w2g, w2u, w3g, w3u,
           xs0, xs1, xs2, accg, accu, hid, hid_s,
           sh_part, sh_recv, gmat, tmat, gcol, csend, crecv, ypart, yrecv, slot_out, wt0, wt1, gpack, pmat,
           l_sem, w_sem, d_sem, snd, r_id, r_x, r_core, r_sh, r_c, r_y):
    me = lax.axis_index("ep")
    tp = lax.axis_index("tp")
    xpeer = lax.rem(me + 2, EP)
    cpeer = me + 1 - 2 * lax.rem(me, 2)
    diag = lax.rem(cpeer + 2, EP)
    xr = (x0, x1, x2)
    xsr = (xs0, xs1, xs2)
    wgr, wur = (w1g, w2g, w3g), (w1u, w2u, w3u)
    mine = pl.ds(pl.multiple_of(me * TOK, TOK), TOK)

    def start(c):
        c.start()
        return c

    def settle(ref, sem):
        pltpu.make_async_copy(ref, ref, sem).wait()

    idc = [start(pltpu.make_async_copy(fid, ids.at[me, 0], l_sem.at[5])),
           start(pltpu.make_async_copy(aid, ids.at[me, 1], l_sem.at[5]))]
    xc = [start(pltpu.make_async_copy(normed.at[:, pl.ds(k, n)], xr[c].at[mine], l_sem.at[0])) for c, (k, n) in enumerate(KC)]
    wrc = start(pltpu.make_async_copy(wr, wr_v, l_sem.at[1]))

    def gu_copy(p, g, i):
        k, n = KC[p]
        src = (weg, weu)[i].at[pl.ds(GRP * g, GRP), :, pl.ds(k, n)]
        return pltpu.make_async_copy(src, (wgr, wur)[i][p].at[pl.ds(GRP * g, GRP)], w_sem.at[p, g])

    def d_buf(j):
        return (w1g, w1u, w2g, w2u, w3g.at[:, :, pl.ds(0, NC)])[j]

    def d_copy(j):
        return pltpu.make_async_copy(wed.at[:, :, pl.ds(j * NC, NC)], d_buf(j), d_sem.at[j])

    def start_pass(p):
        for g in range(NGRP):
            for i in range(2):
                gu_copy(p, g, i).start()


    with scope("barrier"):
        bar = pltpu.get_barrier_semaphore()
        for o in (xpeer, cpeer, diag):
            pl.semaphore_signal(bar, inc=1, device_id={"ep": o}, device_id_type=MESH)
        pl.semaphore_signal(bar, inc=1, device_id={"tp": 1 - tp}, device_id_type=MESH)
        settle(ids.at[0], l_sem.at[5])
        settle(sh_recv, l_sem.at[0])
        swc = [start(pltpu.make_async_copy(s, d, l_sem.at[(2, 3, 6)[i]])) for i, (s, d) in enumerate(((wsg, sg), (wsu, su), (wsd, sd)))]
        pl.semaphore_wait(bar, 4)

    sends = []

    def rcopy(src, dst, r, s, **dev):
        c = pltpu.make_async_remote_copy(src_ref=src, dst_ref=dst, send_sem=snd.at[s], recv_sem=r, device_id=dev, device_id_type=MESH)
        c.start()
        sends.append(c)
        return c

    for d in range(1, EP):
        o = lax.rem(me + d, EP)
        rcopy(ids.at[me], ids.at[me], r_id.at[0], 2, ep=o)
    with scope("xsend"):
        xsend, csnd, fwd = [], [], []
        for c in range(len(KC)):
            xsend.append(rcopy(xr[c].at[mine], xr[c].at[mine], r_x.at[c], 0, ep=xpeer))
        for c in range(len(KC)):
            csnd.append(rcopy(xr[c].at[mine], xr[c].at[mine], r_core.at[c], 0, ep=cpeer))

    theirs = pl.ds(pl.multiple_of(xpeer * TOK, TOK), TOK)

    def forward(c):
        with scope(f"fwait{c}"):
            xsend[c].wait_recv()
        fwd.append(rcopy(xr[c].at[theirs], xr[c].at[theirs], r_core.at[c], 0, ep=cpeer))

    xo = [xr[c][mine, :] for c in range(len(KC))]
    with scope("router"):
        wrc.wait()
        wr_hi = wr_v[...].astype(BF16)
        wr_lo = (wr_v[...] - wr_hi.astype(F32)).astype(BF16)
        logits = jnp.zeros((TOK, EXPERTS), F32)
        for c, (k, kn) in enumerate(KC):
            logits = logits + nt(xo[c], wr_hi[:, k:k + kn]) + nt(xo[c], wr_lo[:, k:k + kn])
        ex = jnp.exp(logits - jnp.max(logits, axis=1, keepdims=True))
        prob = ex / jnp.sum(ex, axis=1, keepdims=True)
    with scope("shwait"):
        swc[0].wait()
        swc[1].wait()
    start_pass(0)
    resc = start(pltpu.make_async_copy(residual, res_v, l_sem.at[4]))
    with scope("shgu"):
        for n0 in range(0, FFS, 256):
            n = min(256, FFS - n0)
            g = sum(nn(xr[c][mine, :], sg[k:k + kn, n0:n0 + n]) for c, (k, kn) in enumerate(KC))
            u = sum(nn(xr[c][mine, :], su[k:k + kn, n0:n0 + n]) for c, (k, kn) in enumerate(KC))
            hid_s[:, n0:n0 + n] = silu_mul(g, u)
    with scope("shdown"):
        swc[2].wait()
        for n0 in range(0, D, 256):
            sh_part[:, n0:n0 + 256] = nn(hid_s[...], sd[:, n0:n0 + 256]).astype(BF16)
    start_pass(1)
    start_pass(2)

    forward(0)
    shc = rcopy(sh_part, sh_recv, r_sh.at[0], 0, tp=1 - tp)

    with scope("idwait"):
        settle(ids.at[pl.ds(0, EP - 1)], r_id.at[0])
    with scope("routing"):
        f = jnp.concatenate([ids[o, 0] for o in range(EP)], axis=1)
        a = jnp.concatenate([ids[o, 1] for o in range(EP)], axis=1)
        ti, tj = lax.broadcasted_iota(I32, (ALL, ALL), 0), lax.broadcasted_iota(I32, (ALL, ALL), 1)
        before = jnp.where(ti < tj, 1.0, 0.0)
        before_dev = jnp.where((ti // TOK) == (tj // TOK), before, 0.0).astype(BF16)
        before = before.astype(BF16)
        eio = lax.broadcasted_iota(I32, (EXPERTS, ALL), 0)
        one_f = jnp.where(eio == f, 1.0, 0.0)
        one_a = jnp.where(eio == a, 1.0, 0.0)
        rank_f = jnp.sum(nn(one_f.astype(BF16), before) * one_f, axis=0, keepdims=True)
        kept = rank_f < CAP - 0.5
        load = jnp.minimum(jnp.sum(one_f, axis=1, keepdims=True), float(CAP))
        over_a = one_a * jnp.where(kept, 0.0, 1.0)
        rank_a = jnp.sum(nn(over_a.astype(BF16), before) * over_a, axis=0, keepdims=True)
        load_a = jnp.sum(one_a * load, axis=0, keepdims=True)
        active = kept | (rank_a + load_a < CAP - 0.5)
        chosen = jnp.where(kept, f, a)
        slot = jnp.where(kept, rank_f, load_a + rank_a).astype(I32)
        owner = chosen // LOCAL
        local = chosen - owner * LOCAL
        here = active & (owner == me)
        slot_code = jnp.where(here, local * SLOT + slot, -1)
        oio = lax.broadcasted_iota(I32, (16, ALL), 0)
        own_f = jnp.where(oio == f // LOCAL, 1.0, 0.0)
        own_a = jnp.where(oio == a // LOCAL + EP, 1.0, 0.0)
        seen = nn((own_f + own_a).astype(BF16), before_dev)
        pos_f = jnp.sum(seen * own_f, axis=0, keepdims=True)
        pos_a = jnp.sum(seen * own_a, axis=0, keepdims=True)
        pos = jnp.where(kept, pos_f, pos_a + PAIR // 2).astype(I32)
        origin = lax.broadcasted_iota(I32, (1, ALL), 1) // TOK
        pair_code = jnp.where(here, origin * PAIR + pos, -1)
        back_code = jnp.where(active, owner * PAIR + pos, -1)
        sio = lax.broadcasted_iota(I32, (SLOTS, ALL), 0)
        smat = jnp.where(sio == slot_code, 1.0, 0.0).astype(BF16)
        rmat = jnp.where(sio == pair_code, 1.0, 0.0).astype(BF16)
        gmat[...] = nt(rmat, smat).astype(BF16)
        pio = lax.broadcasted_iota(I32, (PACK, ALL), 0)
        gpack[...] = nt(rmat, jnp.where(pio == jnp.where(here, local * CAP + slot, -1), 1.0, 0.0).astype(BF16)).astype(BF16)
        col = lax.broadcasted_iota(I32, (PACK, SLOTS), 1)
        packed_row = jnp.where(col % SLOT < CAP, (col // SLOT) * CAP + col % SLOT, -1)
        pmat[...] = jnp.where(lax.broadcasted_iota(I32, (PACK, SLOTS), 0) == packed_row, 1.0, 0.0).astype(BF16)

        own_back, own_chosen = back_code[:, :TOK], jnp.where(active, chosen, -1)[:, :TOK]
        all_chosen = jnp.where(active, chosen, -1)
        for o in range(1, EP):
            cols = slice(o * TOK, (o + 1) * TOK)
            own_back = jnp.where(me == o, back_code[:, cols], own_back)
            own_chosen = jnp.where(me == o, all_chosen[:, cols], own_chosen)
        eye = jnp.where(lax.broadcasted_iota(I32, (TOK, TOK), 0) == lax.broadcasted_iota(I32, (TOK, TOK), 1), 1.0, 0.0).astype(BF16)
        bio = lax.broadcasted_iota(I32, (EP * PAIR, TOK), 0)
        tmat[...] = nt(eye, jnp.where(bio == own_back, 1.0, 0.0).astype(BF16)).astype(BF16)
        cio = lax.broadcasted_iota(I32, (EXPERTS, TOK), 0)
        pick = nt(eye, jnp.where(cio == own_chosen, 1.0, 0.0).astype(BF16))
        gcol[...] = jnp.sum(prob * pick, axis=1, keepdims=True)

    def gather(c):
        with scope(f"xwait{c}"):
            settle(xr[c].at[pl.ds(0, 2 * TOK)], r_core.at[c])
        with scope(f"gather{c}"):
            xsr[c][...] = nn(smat, xr[c][...]).astype(BF16)

    steps = [(p, g) for p in range(len(KC)) for g in range(NGRP)]
    wts = (wt0, wt1)

    def arrived(s):
        p, g = steps[s]
        settle(wgr[p].at[pl.ds(0, 2 * GRP)], w_sem.at[p, g])

    def turn(s, i):
        p, g = steps[s]
        if i < GRP - DIRECT:
            wts[s % 2][i, :KC[p][1], :] = wgr[p][g * GRP + i].T

    def gu_expert(s, i):
        p, g = steps[s]
        n = KC[p][1]
        e = g * GRP + i
        rows = slice(e * SLOT, (e + 1) * SLOT)
        xe = xsr[p][rows, :]
        dg = nn(xe, wts[s % 2][i, :n, :]) if i < GRP - DIRECT else nt(xe, wgr[p][e])
        if p == 0:
            accg[rows, :] = dg
        elif p < len(KC) - 1:
            accg[rows, :] += dg
        for r in range(0, FFE, FFE // 2):
            half = slice(r, r + FFE // 2)
            du = nt(wur[p][e, half, :], xe)
            if p == 0:
                accu[e, half, :] = du
            else:
                accu[e, half, :] += du
        if p == len(KC) - 1:
            hid[rows, :] = silu_mul(accg[rows, :] + dg, accu[e].T)

    def gu_steps(lo, hi):
        with scope(f"gu{lo}"):
            for s in range(lo, hi):
                if s + 1 < len(steps):
                    arrived(s + 1)
            for s in range(lo, hi):
                for i in range(GRP):
                    if s + 1 < len(steps):
                        turn(s + 1, i)
                    gu_expert(s, i)

    arrived(0)
    for i in range(GRP):
        turn(0, i)
    gather(0)
    gu_steps(0, 2)
    forward(1)
    gu_steps(2, 4)
    d_copy(0).start()
    d_copy(1).start()
    gather(1)
    gu_steps(4, 6)
    forward(2)
    gu_steps(6, 8)
    d_copy(2).start()
    d_copy(3).start()
    gather(2)
    for s in range(8, 12):
        gu_steps(s, s + 1)
    d_copy(4).start()

    my_rows = pl.ds(pl.multiple_of(me * PAIR, PAIR), PAIR)

    def go_back(j, rows):
        csend[j] = rows.astype(BF16)
        crecv[j, my_rows, :] = csend[j, my_rows, :]
        out = []
        for d in range(1, EP):
            o = lax.rem(me + d, EP)
            out.append(rcopy(csend.at[j, pl.ds(pl.multiple_of(o * PAIR, PAIR), PAIR)], crecv.at[j, my_rows], r_c.at[j], 1, ep=o))
        return out

    back, over = {}, {}
    for j in range(NCH):
        with scope(f"dw{j}"):
            d_copy(j).wait()
        with scope(f"dn{j}"):
            so, wd = slot_out.at[j % 2], d_buf(j)
            for e in range(LOCAL):
                rows = slice(e * SLOT, (e + 1) * SLOT)
                so[rows, :] = nn(hid[rows, :], wd[e]).astype(BF16)
            if j in TPF:
                ypart[j, :PACK, :] = nn(pmat[...], so[...]).astype(BF16)
                over[j] = rcopy(ypart.at[j, pl.ds(0, PACK)], yrecv.at[j, pl.ds(0, PACK)], r_y.at[j], 1, tp=1 - tp)
            else:
                back[j] = go_back(j, nn(gmat[...], so[...]))

    def first_leg(j):
        if j in TPF:
            with scope(f"fy{j}"):
                over[j].wait_recv()
            r = (ypart[j, :PACK, :].astype(F32) + yrecv[j, :PACK, :].astype(F32)).astype(BF16)
            back[j] = go_back(j, nn(gpack[...], r))
        else:
            with scope(f"fx{j}"):
                settle(crecv.at[j, pl.ds(0, (EP - 1) * PAIR)], r_c.at[j])
            ypart[j, :TOK, :] = nn(tmat[...], crecv[j]).astype(BF16)
            over[j] = rcopy(ypart.at[j, pl.ds(0, TOK)], yrecv.at[j, pl.ds(0, TOK)], r_y.at[j], 1, tp=1 - tp)

    for j in (0, 1, 2, 3, 4):
        first_leg(j)
    with scope("shrecv"):
        resc.wait()
        shc.wait_recv()
    for j in (0, 1, 2, 3, 4):
        cols = slice(j * NC, (j + 1) * NC)
        base = res_v[:, cols].astype(F32) + (sh_part[:, cols].astype(F32) + sh_recv[:, cols].astype(F32))
        with scope(f"last{j}"):
            if j in TPF:
                settle(crecv.at[j, pl.ds(0, (EP - 1) * PAIR)], r_c.at[j])
            else:
                over[j].wait_recv()
        if j in TPF:
            routed = nn(tmat[...], crecv[j])
        else:
            routed = (ypart[j, :TOK, :].astype(F32) + yrecv[j, :TOK, :].astype(F32)).astype(BF16).astype(F32)
        out_ref[:, cols] = (base + gcol[...] * routed).astype(BF16)
    with scope('sendwait'):
        settle(sd.at[pl.ds(0, 4 * TOK)], snd.at[0])
        back_rows = NCH * (EP - 1) * PAIR + len(TPF) * PACK + (NCH - len(TPF)) * TOK
        settle(sd.at[pl.ds(0, back_rows // 2), pl.ds(0, 2 * NC)], snd.at[1])
        settle(ids.at[pl.ds(0, EP - 1)], snd.at[2])


def solution(mesh):
    tok_spec, id_spec = P(("dp", "ep"), None), P(("dp", "ep"))

    def device_step(normed, residual, w_router, ws_gate, ws_up, ws_down, we_gate, we_up, we_down, first_id, alt_id):
        hbm = pl.BlockSpec(memory_space=pl.ANY)
        vm, dma = pltpu.VMEM, pltpu.SemaphoreType.DMA
        weights = [vm((LOCAL, FFE, n), BF16) for _, n in KC for _ in range(2)]
        scratch = [vm((ALL, n), BF16) for _, n in KC]
        scratch += [vm((TOK, D), BF16), vm((EXPERTS, D), F32), vm((EP, 2, 1, TOK), I32)]
        scratch += [vm((D, FFS), BF16), vm((D, FFS), BF16), vm((FFS, D), BF16)] + weights
        scratch += [vm((SLOTS, n), BF16) for _, n in KC]
        scratch += [vm((SLOTS, FFE), F32), vm((LOCAL, FFE, SLOT), F32), vm((SLOTS, FFE), BF16), vm((TOK, FFS), BF16)]
        scratch += [vm((TOK, D), BF16), vm((TOK, D), BF16), vm((EP * PAIR, SLOTS), BF16), vm((TOK, EP * PAIR), BF16), vm((TOK, 1), F32)]
        scratch += [vm((NCH, EP * PAIR, NC), BF16), vm((NCH, EP * PAIR, NC), BF16), vm((NCH, PACK, NC), BF16), vm((NCH, PACK, NC), BF16), vm((2, SLOTS, NC), BF16), vm((GRP - DIRECT, 768, FFE), BF16), vm((GRP - DIRECT, 768, FFE), BF16), vm((EP * PAIR, PACK), BF16), vm((PACK, SLOTS), BF16)]
        scratch += [dma((7,)), dma((len(KC), NGRP)), dma((NCH,)), dma((3,)), dma((1,)), dma((len(KC),)), dma((len(KC),)), dma((1,)), dma((NCH,)), dma((NCH,))]
        return pl.pallas_call(
            kernel,
            out_shape=pltpu.VMEM((TOK, D), BF16),
            in_specs=[hbm] * 11,
            out_specs=pl.BlockSpec(memory_space=pltpu.VMEM),
            scratch_shapes=scratch,
            compiler_params=pltpu.CompilerParams(collective_id=0, has_side_effects=True, vmem_limit_bytes=65_000_000),
            name="moe_layer",
        )(normed, residual, w_router.T, ws_gate, ws_up, ws_down, jnp.swapaxes(we_gate, 1, 2), jnp.swapaxes(we_up, 1, 2), we_down,
          first_id.reshape(1, TOK), alt_id.reshape(1, TOK))

    return jax.shard_map(device_step, mesh=mesh,
                         in_specs=(tok_spec, tok_spec, P(None, None), P(None, "tp"), P(None, "tp"), P("tp", None), P("ep", None, "tp"),
                                   P("ep", None, "tp"), P("ep", "tp", None), id_spec, id_spec),
                         out_specs=tok_spec, check_vma=False)
```

```python
import functools

import jax
import jax.numpy as jnp
from jax import lax
from jax.experimental import pallas as pl
from jax.experimental.pallas import tpu as pltpu
from jax.sharding import PartitionSpec as P

MESH = pl.DeviceIdType.MESH
scope = jax.named_scope
F32, BF16, I32 = jnp.float32, jnp.bfloat16, jnp.int32

EP = 4
TOK = 128
ALL = EP * TOK
EXPERTS = 64
LOCAL = EXPERTS // EP
CAP = 10
SLOT = 16
SLOTS = LOCAL * SLOT
PAIR = 64
D = 1280
FFE = 448
FFS = 896
GRP = 4
NGRP = LOCAL // GRP
DIRECT = 1
KC = tuple((k, 256) for k in range(0, D, 256))
NC = 256
NCH = D // NC
TPF = (1, 3)
PACK = LOCAL * CAP


def nn(a, b):
    return lax.dot_general(a, b, (((1,), (0,)), ((), ())), preferred_element_type=F32)


def nt(a, b):
    return lax.dot_general(a, b, (((1,), (1,)), ((), ())), preferred_element_type=F32)


def silu_mul(g, u):
    return (g * (1.0 / (1.0 + jnp.exp(-g))) * u).astype(BF16)


def kernel(normed, residual, wr, wsg, wsu, wsd, weg, weu, wed, fid, aid, out_ref,
           x0, x1, x2, x3, x4, res_v, wr_v, ids,
           sg, su, sd, w1g, w1u, w2g, w2u, w3g, w3u, w4g, w4u, w5g, w5u,
           xs0, xs1, xs2, xs3, xs4, accg, accu, hid, hid_s,
           sh_part, sh_recv, gmat, tmat, gcol, csend, crecv, ypart, yrecv, slot_out, wt0, wt1, gpack, pmat,
           l_sem, w_sem, d_sem, snd, r_id, r_x, r_core, r_sh, r_c, r_y):
    me = lax.axis_index("ep")
    tp = lax.axis_index("tp")
    xpeer = lax.rem(me + 2, EP)
    cpeer = me + 1 - 2 * lax.rem(me, 2)
    diag = lax.rem(cpeer + 2, EP)
    xr = (x0, x1, x2, x3, x4)
    xsr = (xs0, xs1, xs2, xs3, xs4)
    wgr, wur = (w1g, w2g, w3g, w4g, w5g), (w1u, w2u, w3u, w4u, w5u)
    mine = pl.ds(pl.multiple_of(me * TOK, TOK), TOK)

    def start(c):
        c.start()
        return c

    def settle(ref, sem):
        pltpu.make_async_copy(ref, ref, sem).wait()

    idc = [start(pltpu.make_async_copy(fid, ids.at[me, 0], l_sem.at[5])),
           start(pltpu.make_async_copy(aid, ids.at[me, 1], l_sem.at[5]))]
    xc = [start(pltpu.make_async_copy(normed.at[:, pl.ds(k, n)], xr[c].at[mine], l_sem.at[0])) for c, (k, n) in enumerate(KC)]
    wrc = start(pltpu.make_async_copy(wr, wr_v, l_sem.at[1]))

    def gu_copy(p, h, i):
        k, n = KC[p]
        part = pl.ds(2 * GRP * h, 2 * GRP)
        return pltpu.make_async_copy((weg, weu)[i].at[part, :, pl.ds(k, n)], (wgr, wur)[i][p].at[part], w_sem.at[p, h])

    def d_buf(j):
        return (w1g, w1u, w2g, w2u, w3g)[j]

    def d_copy(j):
        return pltpu.make_async_copy(wed.at[:, :, pl.ds(j * NC, NC)], d_buf(j), d_sem.at[j])

    def start_pass(p):
        for h in range(NGRP // 2):
            for i in range(2):
                gu_copy(p, h, i).start()

    with scope("barrier"):
        bar = pltpu.get_barrier_semaphore()
        for o in (xpeer, cpeer, diag):
            pl.semaphore_signal(bar, inc=1, device_id={"ep": o}, device_id_type=MESH)
        pl.semaphore_signal(bar, inc=1, device_id={"tp": 1 - tp}, device_id_type=MESH)
        settle(ids.at[0], l_sem.at[5])
        settle(sh_recv, l_sem.at[0])
        swc = [start(pltpu.make_async_copy(s, d, l_sem.at[(2, 3, 6)[i]])) for i, (s, d) in enumerate(((wsg, sg), (wsu, su), (wsd, sd)))]
        pl.semaphore_wait(bar, 4)

    sends = []

    def rcopy(src, dst, r, s, **dev):
        c = pltpu.make_async_remote_copy(src_ref=src, dst_ref=dst, send_sem=snd.at[s], recv_sem=r, device_id=dev, device_id_type=MESH)
        c.start()
        sends.append(c)
        return c

    for d in range(1, EP):
        o = lax.rem(me + d, EP)
        rcopy(ids.at[me], ids.at[me], r_id.at[0], 2, ep=o)
    with scope("xsend"):
        xsend, csnd, fwd = [], [], []
        for c in range(len(KC)):
            xsend.append(rcopy(xr[c].at[mine], xr[c].at[mine], r_x.at[c], 0, ep=xpeer))
        for c in range(len(KC)):
            csnd.append(rcopy(xr[c].at[mine], xr[c].at[mine], r_core.at[c], 0, ep=cpeer))

    start_pass(0)
    theirs = pl.ds(pl.multiple_of(xpeer * TOK, TOK), TOK)

    def forward(c):
        with scope(f"fwait{c}"):
            xsend[c].wait_recv()
        fwd.append(rcopy(xr[c].at[theirs], xr[c].at[theirs], r_core.at[c], 0, ep=cpeer))

    xo = [xr[c][mine, :] for c in range(len(KC))]
    with scope("router"):
        wrc.wait()
        wr_hi = wr_v[...].astype(BF16)
        wr_lo = (wr_v[...] - wr_hi.astype(F32)).astype(BF16)
        logits = jnp.zeros((TOK, EXPERTS), F32)
        for c, (k, kn) in enumerate(KC):
            logits = logits + nt(xo[c], wr_hi[:, k:k + kn]) + nt(xo[c], wr_lo[:, k:k + kn])
        ex = jnp.exp(logits - jnp.max(logits, axis=1, keepdims=True))
        prob = ex / jnp.sum(ex, axis=1, keepdims=True)
    with scope("shwait"):
        swc[0].wait()
        swc[1].wait()
    resc = start(pltpu.make_async_copy(residual, res_v, l_sem.at[4]))
    with scope("shgu"):
        for n0 in range(0, FFS, 256):
            n = min(256, FFS - n0)
            g = sum(nn(xr[c][mine, :], sg[k:k + kn, n0:n0 + n]) for c, (k, kn) in enumerate(KC))
            u = sum(nn(xr[c][mine, :], su[k:k + kn, n0:n0 + n]) for c, (k, kn) in enumerate(KC))
            hid_s[:, n0:n0 + n] = silu_mul(g, u)
    with scope("shdown"):
        swc[2].wait()
        for n0 in range(0, D, 256):
            sh_part[:, n0:n0 + 256] = nn(hid_s[...], sd[:, n0:n0 + 256]).astype(BF16)
    start_pass(1)
    start_pass(2)

    forward(0)
    shc = rcopy(sh_part, sh_recv, r_sh.at[0], 0, tp=1 - tp)

    with scope("idwait"):
        settle(ids.at[pl.ds(0, EP - 1)], r_id.at[0])
    with scope("routing"):
        f = jnp.concatenate([ids[o, 0] for o in range(EP)], axis=1)
        a = jnp.concatenate([ids[o, 1] for o in range(EP)], axis=1)
        ti, tj = lax.broadcasted_iota(I32, (ALL, ALL), 0), lax.broadcasted_iota(I32, (ALL, ALL), 1)
        before = jnp.where(ti < tj, 1.0, 0.0)
        before_dev = jnp.where((ti // TOK) == (tj // TOK), before, 0.0).astype(BF16)
        before = before.astype(BF16)
        eio = lax.broadcasted_iota(I32, (EXPERTS, ALL), 0)
        one_f = jnp.where(eio == f, 1.0, 0.0)
        one_a = jnp.where(eio == a, 1.0, 0.0)
        rank_f = jnp.sum(nn(one_f.astype(BF16), before) * one_f, axis=0, keepdims=True)
        kept = rank_f < CAP - 0.5
        load = jnp.minimum(jnp.sum(one_f, axis=1, keepdims=True), float(CAP))
        over_a = one_a * jnp.where(kept, 0.0, 1.0)
        rank_a = jnp.sum(nn(over_a.astype(BF16), before) * over_a, axis=0, keepdims=True)
        load_a = jnp.sum(one_a * load, axis=0, keepdims=True)
        active = kept | (rank_a + load_a < CAP - 0.5)
        chosen = jnp.where(kept, f, a)
        slot = jnp.where(kept, rank_f, load_a + rank_a).astype(I32)
        owner = chosen // LOCAL
        local = chosen - owner * LOCAL
        here = active & (owner == me)
        slot_code = jnp.where(here, local * SLOT + slot, -1)
        oio = lax.broadcasted_iota(I32, (16, ALL), 0)
        own_f = jnp.where(oio == f // LOCAL, 1.0, 0.0)
        own_a = jnp.where(oio == a // LOCAL + EP, 1.0, 0.0)
        seen = nn((own_f + own_a).astype(BF16), before_dev)
        pos_f = jnp.sum(seen * own_f, axis=0, keepdims=True)
        pos_a = jnp.sum(seen * own_a, axis=0, keepdims=True)
        pos = jnp.where(kept, pos_f, pos_a + PAIR // 2).astype(I32)
        origin = lax.broadcasted_iota(I32, (1, ALL), 1) // TOK
        pair_code = jnp.where(here, origin * PAIR + pos, -1)
        back_code = jnp.where(active, owner * PAIR + pos, -1)
        sio = lax.broadcasted_iota(I32, (SLOTS, ALL), 0)
        smat = jnp.where(sio == slot_code, 1.0, 0.0).astype(BF16)
        rmat = jnp.where(sio == pair_code, 1.0, 0.0).astype(BF16)
        gmat[...] = nt(rmat, smat).astype(BF16)
        pio = lax.broadcasted_iota(I32, (PACK, ALL), 0)
        gpack[...] = nt(rmat, jnp.where(pio == jnp.where(here, local * CAP + slot, -1), 1.0, 0.0).astype(BF16)).astype(BF16)
        col = lax.broadcasted_iota(I32, (PACK, SLOTS), 1)
        packed_row = jnp.where(col % SLOT < CAP, (col // SLOT) * CAP + col % SLOT, -1)
        pmat[...] = jnp.where(lax.broadcasted_iota(I32, (PACK, SLOTS), 0) == packed_row, 1.0, 0.0).astype(BF16)

        own_back, own_chosen = back_code[:, :TOK], jnp.where(active, chosen, -1)[:, :TOK]
        all_chosen = jnp.where(active, chosen, -1)
        for o in range(1, EP):
            cols = slice(o * TOK, (o + 1) * TOK)
            own_back = jnp.where(me == o, back_code[:, cols], own_back)
            own_chosen = jnp.where(me == o, all_chosen[:, cols], own_chosen)
        eye = jnp.where(lax.broadcasted_iota(I32, (TOK, TOK), 0) == lax.broadcasted_iota(I32, (TOK, TOK), 1), 1.0, 0.0).astype(BF16)
        bio = lax.broadcasted_iota(I32, (EP * PAIR, TOK), 0)
        tmat[...] = nt(eye, jnp.where(bio == own_back, 1.0, 0.0).astype(BF16)).astype(BF16)
        cio = lax.broadcasted_iota(I32, (EXPERTS, TOK), 0)
        pick = nt(eye, jnp.where(cio == own_chosen, 1.0, 0.0).astype(BF16))
        gcol[...] = jnp.sum(prob * pick, axis=1, keepdims=True)

    def gather(c):
        with scope(f"xwait{c}"):
            settle(xr[c].at[pl.ds(0, 2 * TOK)], r_core.at[c])
        with scope(f"gather{c}"):
            xsr[c][...] = nn(smat, xr[c][...]).astype(BF16)

    steps = [(p, g) for p in range(len(KC)) for g in range(NGRP)]
    wts = (wt0, wt1)

    def arrived(s):
        p, g = steps[s]
        if g % 2 == 0:
            settle(wgr[p], w_sem.at[p, g // 2])

    def turn(s, i):
        p, g = steps[s]
        if i < GRP - DIRECT:
            wts[s % 2][i, :KC[p][1], :] = wgr[p][g * GRP + i].T

    def gu_expert(s, i):
        p, g = steps[s]
        n = KC[p][1]
        e = g * GRP + i
        rows = slice(e * SLOT, (e + 1) * SLOT)
        xe = xsr[p][rows, :]
        dg = nn(xe, wts[s % 2][i, :n, :]) if i < GRP - DIRECT else nt(xe, wgr[p][e])
        if p == 0:
            accg[rows, :] = dg
        elif p < len(KC) - 1:
            accg[rows, :] += dg
        for r in range(0, FFE, FFE // 2):
            half = slice(r, r + FFE // 2)
            du = nt(wur[p][e, half, :], xe)
            if p == 0:
                accu[e, half, :] = du
            else:
                accu[e, half, :] += du
        if p == len(KC) - 1:
            hid[rows, :] = silu_mul(accg[rows, :] + dg, accu[e].T)

    def gu_steps(lo, hi):
        with scope(f"gu{lo}"):
            for s in range(lo, hi):
                if s + 1 < len(steps):
                    arrived(s + 1)
            for s in range(lo, hi):
                for i in range(GRP):
                    if s + 1 < len(steps):
                        turn(s + 1, i)
                    gu_expert(s, i)

    arrived(0)
    for i in range(GRP):
        turn(0, i)
    gather(0)
    for p in range(len(KC)):
        if p > 0:
            gather(p)
        gu_steps(NGRP * p, NGRP * p + 2)
        if p + 1 < len(KC):
            forward(p + 1)
        gu_steps(NGRP * p + 2, NGRP * p + 4)
        if p < 2:
            start_pass(p + 3)
        for j in {1: (0, 1), 2: (2, 3), 3: (4,)}.get(p, ()):
            d_copy(j).start()

    my_rows = pl.ds(pl.multiple_of(me * PAIR, PAIR), PAIR)

    def go_back(j, rows):
        csend[j] = rows.astype(BF16)
        crecv[j, my_rows, :] = csend[j, my_rows, :]
        out = []
        for d in range(1, EP):
            o = lax.rem(me + d, EP)
            out.append(rcopy(csend.at[j, pl.ds(pl.multiple_of(o * PAIR, PAIR), PAIR)], crecv.at[j, my_rows], r_c.at[j], 1, ep=o))
        return out

    back, over = {}, {}
    for j in range(NCH):
        with scope(f"dw{j}"):
            d_copy(j).wait()
        with scope(f"dn{j}"):
            so, wd = slot_out.at[j % 2], d_buf(j)
            for e in range(LOCAL):
                rows = slice(e * SLOT, (e + 1) * SLOT)
                so[rows, :] = nn(hid[rows, :], wd[e]).astype(BF16)
            if j in TPF:
                ypart[j, :PACK, :] = nn(pmat[...], so[...]).astype(BF16)
                over[j] = rcopy(ypart.at[j, pl.ds(0, PACK)], yrecv.at[j, pl.ds(0, PACK)], r_y.at[j], 1, tp=1 - tp)
            else:
                back[j] = go_back(j, nn(gmat[...], so[...]))

    def first_leg(j):
        if j in TPF:
            with scope(f"fy{j}"):
                over[j].wait_recv()
            r = (ypart[j, :PACK, :].astype(F32) + yrecv[j, :PACK, :].astype(F32)).astype(BF16)
            back[j] = go_back(j, nn(gpack[...], r))
        else:
            with scope(f"fx{j}"):
                settle(crecv.at[j, pl.ds(0, (EP - 1) * PAIR)], r_c.at[j])
            ypart[j, :TOK, :] = nn(tmat[...], crecv[j]).astype(BF16)
            over[j] = rcopy(ypart.at[j, pl.ds(0, TOK)], yrecv.at[j, pl.ds(0, TOK)], r_y.at[j], 1, tp=1 - tp)

    for j in (0, 1, 2, 3, 4):
        first_leg(j)
    with scope("shrecv"):
        resc.wait()
        shc.wait_recv()
    for j in (0, 1, 2, 3, 4):
        cols = slice(j * NC, (j + 1) * NC)
        base = res_v[:, cols].astype(F32) + (sh_part[:, cols].astype(F32) + sh_recv[:, cols].astype(F32))
        with scope(f"last{j}"):
            if j in TPF:
                settle(crecv.at[j, pl.ds(0, (EP - 1) * PAIR)], r_c.at[j])
            else:
                over[j].wait_recv()
        if j in TPF:
            routed = nn(tmat[...], crecv[j])
        else:
            routed = (ypart[j, :TOK, :].astype(F32) + yrecv[j, :TOK, :].astype(F32)).astype(BF16).astype(F32)
        out_ref[:, cols] = (base + gcol[...] * routed).astype(BF16)
    with scope('sendwait'):
        settle(sd.at[pl.ds(0, 4 * TOK)], snd.at[0])
        back_rows = NCH * (EP - 1) * PAIR + len(TPF) * PACK + (NCH - len(TPF)) * TOK
        settle(sd.at[pl.ds(0, back_rows // 2), pl.ds(0, 2 * NC)], snd.at[1])
        settle(ids.at[pl.ds(0, EP - 1)], snd.at[2])


def solution(mesh):
    tok_spec, id_spec = P(("dp", "ep"), None), P(("dp", "ep"))

    def device_step(normed, residual, w_router, ws_gate, ws_up, ws_down, we_gate, we_up, we_down, first_id, alt_id):
        hbm = pl.BlockSpec(memory_space=pl.ANY)
        vm, dma = pltpu.VMEM, pltpu.SemaphoreType.DMA
        weights = [vm((LOCAL, FFE, n), BF16) for _, n in KC for _ in range(2)]
        scratch = [vm((ALL, n), BF16) for _, n in KC]
        scratch += [vm((TOK, D), BF16), vm((EXPERTS, D), F32), vm((EP, 2, 1, TOK), I32)]
        scratch += [vm((D, FFS), BF16), vm((D, FFS), BF16), vm((FFS, D), BF16)] + weights
        scratch += [vm((SLOTS, n), BF16) for _, n in KC]
        scratch += [vm((SLOTS, FFE), F32), vm((LOCAL, FFE, SLOT), F32), vm((SLOTS, FFE), BF16), vm((TOK, FFS), BF16)]
        scratch += [vm((TOK, D), BF16), vm((TOK, D), BF16), vm((EP * PAIR, SLOTS), BF16), vm((TOK, EP * PAIR), BF16), vm((TOK, 1), F32)]
        scratch += [vm((NCH, EP * PAIR, NC), BF16), vm((NCH, EP * PAIR, NC), BF16), vm((NCH, PACK, NC), BF16), vm((NCH, PACK, NC), BF16), vm((2, SLOTS, NC), BF16), vm((GRP - DIRECT, 256, FFE), BF16), vm((GRP - DIRECT, 256, FFE), BF16), vm((EP * PAIR, PACK), BF16), vm((PACK, SLOTS), BF16)]
        scratch += [dma((7,)), dma((len(KC), NGRP // 2)), dma((NCH,)), dma((3,)), dma((1,)), dma((len(KC),)), dma((len(KC),)), dma((1,)), dma((NCH,)), dma((NCH,))]
        return pl.pallas_call(
            kernel,
            out_shape=pltpu.VMEM((TOK, D), BF16),
            in_specs=[hbm] * 11,
            out_specs=pl.BlockSpec(memory_space=pltpu.VMEM),
            scratch_shapes=scratch,
            compiler_params=pltpu.CompilerParams(collective_id=0, has_side_effects=True, vmem_limit_bytes=65_000_000),
            name="moe_layer",
        )(normed, residual, w_router.T, ws_gate, ws_up, ws_down, jnp.swapaxes(we_gate, 1, 2), jnp.swapaxes(we_up, 1, 2), we_down,
          first_id.reshape(1, TOK), alt_id.reshape(1, TOK))

    return jax.shard_map(device_step, mesh=mesh,
                         in_specs=(tok_spec, tok_spec, P(None, None), P(None, "tp"), P(None, "tp"), P("tp", None), P("ep", None, "tp"),
                                   P("ep", None, "tp"), P("ep", "tp", None), id_spec, id_spec),
                         out_specs=tok_spec, check_vma=False)
```

```python
import functools

import jax
import jax.numpy as jnp
from jax import lax
from jax.experimental import pallas as pl
from jax.experimental.pallas import tpu as pltpu
from jax.sharding import PartitionSpec as P

MESH = pl.DeviceIdType.MESH
scope = jax.named_scope
F32, BF16, I32 = jnp.float32, jnp.bfloat16, jnp.int32

EP = 4
TOK = 128
ALL = EP * TOK
EXPERTS = 64
LOCAL = EXPERTS // EP
CAP = 10
SLOT = 16
SLOTS = LOCAL * SLOT
PAIR = 64
D = 1280
FFE = 448
FFS = 896
GRP = 4
NGRP = LOCAL // GRP
DIRECT = 1
KC = tuple((k, 256) for k in range(0, D, 256))
NC = 256
NCH = D // NC
TPF = (1, 3)
PACK = LOCAL * CAP


def nn(a, b):
    return lax.dot_general(a, b, (((1,), (0,)), ((), ())), preferred_element_type=F32)


def nt(a, b):
    return lax.dot_general(a, b, (((1,), (1,)), ((), ())), preferred_element_type=F32)


def silu_mul(g, u):
    return (g * (1.0 / (1.0 + jnp.exp(-g))) * u).astype(BF16)


def kernel(normed, residual, wr, wsg, wsu, wsd, weg, weu, wed, fid, aid, out_ref,
           x0, x1, x2, x3, x4, res_v, wr_v, ids,
           sg, su, sd, w1g, w1u, w2g, w2u, w3g, w3u, w4g, w4u, w5g, w5u,
           xs0, xs1, xs2, xs3, xs4, accg, accu, hid, hid_s,
           sh_part, sh_recv, gmat, tmat, gcol, csend, crecv, ypart, yrecv, slot_out, wt0, wt1, gpack, pmat,
           l_sem, w_sem, d_sem, snd, r_id, r_x, r_core, r_sh, r_c, r_y):
    me = lax.axis_index("ep")
    tp = lax.axis_index("tp")
    xpeer = lax.rem(me + 2, EP)
    cpeer = me + 1 - 2 * lax.rem(me, 2)
    diag = lax.rem(cpeer + 2, EP)
    xr = (x0, x1, x2, x3, x4)
    xsr = (xs0, xs1, xs2, xs3, xs4)
    wgr, wur = (w1g, w2g, w3g, w4g, w5g), (w1u, w2u, w3u, w4u, w5u)
    mine = pl.ds(pl.multiple_of(me * TOK, TOK), TOK)

    def start(c):
        c.start()
        return c

    def settle(ref, sem):
        pltpu.make_async_copy(ref, ref, sem).wait()

    idc = [start(pltpu.make_async_copy(fid, ids.at[me, 0], l_sem.at[5])),
           start(pltpu.make_async_copy(aid, ids.at[me, 1], l_sem.at[5]))]
    xc = [start(pltpu.make_async_copy(normed.at[:, pl.ds(k, n)], xr[c].at[mine], l_sem.at[0])) for c, (k, n) in enumerate(KC)]
    wrc = start(pltpu.make_async_copy(wr, wr_v, l_sem.at[1]))

    def gu_copy(p, h, i):
        k, n = KC[p]
        part = pl.ds(2 * GRP * h, 2 * GRP)
        return pltpu.make_async_copy((weg, weu)[i].at[part, :, pl.ds(k, n)], (wgr, wur)[i][p].at[part], w_sem.at[p, h])

    def d_buf(j):
        return (w1g, w1u, w2g, w2u, w3g)[j]

    def d_copy(j):
        return pltpu.make_async_copy(wed.at[:, :, pl.ds(j * NC, NC)], d_buf(j), d_sem.at[j])

    def start_pass(p):
        for h in range(NGRP // 2):
            for i in range(2):
                gu_copy(p, h, i).start()

    with scope("barrier"):
        bar = pltpu.get_barrier_semaphore()
        for o in (xpeer, cpeer, diag):
            pl.semaphore_signal(bar, inc=1, device_id={"ep": o}, device_id_type=MESH)
        pl.semaphore_signal(bar, inc=1, device_id={"tp": 1 - tp}, device_id_type=MESH)
        settle(ids.at[0], l_sem.at[5])
        settle(sh_recv, l_sem.at[0])
        swc = [start(pltpu.make_async_copy(s, d, l_sem.at[(2, 3, 6)[i]])) for i, (s, d) in enumerate(((wsg, sg), (wsu, su), (wsd, sd)))]
        pl.semaphore_wait(bar, 4)

    sends = []

    def rcopy(src, dst, r, s, **dev):
        c = pltpu.make_async_remote_copy(src_ref=src, dst_ref=dst, send_sem=snd.at[s], recv_sem=r, device_id=dev, device_id_type=MESH)
        c.start()
        sends.append(c)
        return c

    for d in range(1, EP):
        o = lax.rem(me + d, EP)
        rcopy(ids.at[me], ids.at[me], r_id.at[0], 2, ep=o)
    with scope("xsend"):
        xsend, csnd, fwd = [], [], []
        for c in range(len(KC)):
            xsend.append(rcopy(xr[c].at[mine], xr[c].at[mine], r_x.at[c], 0, ep=xpeer))
        for c in range(len(KC)):
            csnd.append(rcopy(xr[c].at[mine], xr[c].at[mine], r_core.at[c], 0, ep=cpeer))

    start_pass(0)
    theirs = pl.ds(pl.multiple_of(xpeer * TOK, TOK), TOK)

    def forward(c):
        with scope(f"fwait{c}"):
            xsend[c].wait_recv()
        fwd.append(rcopy(xr[c].at[theirs], xr[c].at[theirs], r_core.at[c], 0, ep=cpeer))

    xo = [xr[c][mine, :] for c in range(len(KC))]
    with scope("router"):
        wrc.wait()
        wr_hi = wr_v[...].astype(BF16)
        wr_lo = (wr_v[...] - wr_hi.astype(F32)).astype(BF16)
        logits = jnp.zeros((TOK, EXPERTS), F32)
        for c, (k, kn) in enumerate(KC):
            logits = logits + nt(xo[c], wr_hi[:, k:k + kn]) + nt(xo[c], wr_lo[:, k:k + kn])
        ex = jnp.exp(logits - jnp.max(logits, axis=1, keepdims=True))
        prob = ex / jnp.sum(ex, axis=1, keepdims=True)
    with scope("shwait"):
        swc[0].wait()
        swc[1].wait()
    resc = start(pltpu.make_async_copy(residual, res_v, l_sem.at[4]))
    with scope("shgu"):
        for n0 in range(0, FFS, 256):
            n = min(256, FFS - n0)
            g = sum(nn(xr[c][mine, :], sg[k:k + kn, n0:n0 + n]) for c, (k, kn) in enumerate(KC))
            u = sum(nn(xr[c][mine, :], su[k:k + kn, n0:n0 + n]) for c, (k, kn) in enumerate(KC))
            hid_s[:, n0:n0 + n] = silu_mul(g, u)
    with scope("shdown"):
        swc[2].wait()
        for n0 in range(0, D, 256):
            sh_part[:, n0:n0 + 256] = nn(hid_s[...], sd[:, n0:n0 + 256]).astype(BF16)
    start_pass(1)
    start_pass(2)

    forward(0)
    shc = rcopy(sh_part, sh_recv, r_sh.at[0], 0, tp=1 - tp)

    with scope("idwait"):
        settle(ids.at[pl.ds(0, EP - 1)], r_id.at[0])
    with scope("routing"):
        f = jnp.concatenate([ids[o, 0] for o in range(EP)], axis=1)
        a = jnp.concatenate([ids[o, 1] for o in range(EP)], axis=1)
        ti, tj = lax.broadcasted_iota(I32, (ALL, ALL), 0), lax.broadcasted_iota(I32, (ALL, ALL), 1)
        before = jnp.where(ti < tj, 1.0, 0.0)
        before_dev = jnp.where((ti // TOK) == (tj // TOK), before, 0.0).astype(BF16)
        before = before.astype(BF16)
        eio = lax.broadcasted_iota(I32, (EXPERTS, ALL), 0)
        one_f = jnp.where(eio == f, 1.0, 0.0)
        one_a = jnp.where(eio == a, 1.0, 0.0)
        rank_f = jnp.sum(nn(one_f.astype(BF16), before) * one_f, axis=0, keepdims=True)
        kept = rank_f < CAP - 0.5
        load = jnp.minimum(jnp.sum(one_f, axis=1, keepdims=True), float(CAP))
        over_a = one_a * jnp.where(kept, 0.0, 1.0)
        rank_a = jnp.sum(nn(over_a.astype(BF16), before) * over_a, axis=0, keepdims=True)
        load_a = jnp.sum(one_a * load, axis=0, keepdims=True)
        active = kept | (rank_a + load_a < CAP - 0.5)
        chosen = jnp.where(kept, f, a)
        slot = jnp.where(kept, rank_f, load_a + rank_a).astype(I32)
        owner = chosen // LOCAL
        local = chosen - owner * LOCAL
        here = active & (owner == me)
        slot_code = jnp.where(here, local * SLOT + slot, -1)
        oio = lax.broadcasted_iota(I32, (16, ALL), 0)
        own_f = jnp.where(oio == f // LOCAL, 1.0, 0.0)
        own_a = jnp.where(oio == a // LOCAL + EP, 1.0, 0.0)
        seen = nn((own_f + own_a).astype(BF16), before_dev)
        pos_f = jnp.sum(seen * own_f, axis=0, keepdims=True)
        pos_a = jnp.sum(seen * own_a, axis=0, keepdims=True)
        pos = jnp.where(kept, pos_f, pos_a + PAIR // 2).astype(I32)
        origin = lax.broadcasted_iota(I32, (1, ALL), 1) // TOK
        pair_code = jnp.where(here, origin * PAIR + pos, -1)
        back_code = jnp.where(active, owner * PAIR + pos, -1)
        sio = lax.broadcasted_iota(I32, (SLOTS, ALL), 0)
        smat = jnp.where(sio == slot_code, 1.0, 0.0).astype(BF16)
        rmat = jnp.where(sio == pair_code, 1.0, 0.0).astype(BF16)
        gmat[...] = nt(rmat, smat).astype(BF16)
        pio = lax.broadcasted_iota(I32, (PACK, ALL), 0)
        gpack[...] = nt(rmat, jnp.where(pio == jnp.where(here, local * CAP + slot, -1), 1.0, 0.0).astype(BF16)).astype(BF16)
        col = lax.broadcasted_iota(I32, (PACK, SLOTS), 1)
        packed_row = jnp.where(col % SLOT < CAP, (col // SLOT) * CAP + col % SLOT, -1)
        pmat[...] = jnp.where(lax.broadcasted_iota(I32, (PACK, SLOTS), 0) == packed_row, 1.0, 0.0).astype(BF16)

        own_back, own_chosen = back_code[:, :TOK], jnp.where(active, chosen, -1)[:, :TOK]
        all_chosen = jnp.where(active, chosen, -1)
        for o in range(1, EP):
            cols = slice(o * TOK, (o + 1) * TOK)
            own_back = jnp.where(me == o, back_code[:, cols], own_back)
            own_chosen = jnp.where(me == o, all_chosen[:, cols], own_chosen)
        eye = jnp.where(lax.broadcasted_iota(I32, (TOK, TOK), 0) == lax.broadcasted_iota(I32, (TOK, TOK), 1), 1.0, 0.0).astype(BF16)
        bio = lax.broadcasted_iota(I32, (EP * PAIR, TOK), 0)
        tmat[...] = nt(eye, jnp.where(bio == own_back, 1.0, 0.0).astype(BF16)).astype(BF16)
        cio = lax.broadcasted_iota(I32, (EXPERTS, TOK), 0)
        pick = nt(eye, jnp.where(cio == own_chosen, 1.0, 0.0).astype(BF16))
        gcol[...] = jnp.sum(prob * pick, axis=1, keepdims=True)

    def gather(c):
        with scope(f"xwait{c}"):
            settle(xr[c].at[pl.ds(0, 2 * TOK)], r_core.at[c])
        with scope(f"gather{c}"):
            xsr[c][...] = nn(smat, xr[c][...]).astype(BF16)

    steps = [(p, g) for p in range(len(KC)) for g in range(NGRP)]
    wts = (wt0, wt1)

    def arrived(s):
        p, g = steps[s]
        if g % 2 == 0:
            settle(wgr[p], w_sem.at[p, g // 2])

    def turn(s, i):
        p, g = steps[s]
        if i < GRP - DIRECT:
            wts[s % 2][i, :KC[p][1], :] = wgr[p][g * GRP + i].T

    def gu_expert(s, i):
        p, g = steps[s]
        n = KC[p][1]
        e = g * GRP + i
        rows = slice(e * SLOT, (e + 1) * SLOT)
        xe = xsr[p][rows, :]
        dg = nn(xe, wts[s % 2][i, :n, :]) if i < GRP - DIRECT else nt(xe, wgr[p][e])
        if p == 0:
            accg[rows, :] = dg
        elif p < len(KC) - 1:
            accg[rows, :] += dg
        for r in range(0, FFE, FFE // 2):
            half = slice(r, r + FFE // 2)
            du = nt(wur[p][e, half, :], xe)
            if p == 0:
                accu[e, half, :] = du
            else:
                accu[e, half, :] += du
        if p == len(KC) - 1:
            hid[rows, :] = silu_mul(accg[rows, :] + dg, accu[e].T)

    def gu_steps(lo, hi):
        with scope(f"gu{lo}"):
            for s in range(lo, hi):
                if s + 1 < len(steps):
                    arrived(s + 1)
            for s in range(lo, hi):
                for i in range(GRP):
                    if s + 1 < len(steps):
                        turn(s + 1, i)
                    gu_expert(s, i)

    arrived(0)
    for i in range(GRP):
        turn(0, i)
    gather(0)
    for p in range(len(KC)):
        if p > 0:
            gather(p)
        if p + 1 < len(KC):
            forward(p + 1)
        gu_steps(NGRP * p, NGRP * p + 2)
        gu_steps(NGRP * p + 2, NGRP * p + 4)
        if p < 2:
            start_pass(p + 3)
        for j in {1: (0, 1), 2: (2, 3), 3: (4,)}.get(p, ()):
            d_copy(j).start()

    my_rows = pl.ds(pl.multiple_of(me * PAIR, PAIR), PAIR)

    def go_back(j, rows):
        csend[j] = rows.astype(BF16)
        crecv[j, my_rows, :] = csend[j, my_rows, :]
        out = []
        for d in range(1, EP):
            o = lax.rem(me + d, EP)
            out.append(rcopy(csend.at[j, pl.ds(pl.multiple_of(o * PAIR, PAIR), PAIR)], crecv.at[j, my_rows], r_c.at[j], 1, ep=o))
        return out

    back, over = {}, {}
    for j in range(NCH):
        with scope(f"dw{j}"):
            d_copy(j).wait()
        with scope(f"dn{j}"):
            so, wd = slot_out.at[j % 2], d_buf(j)
            for e in range(LOCAL):
                rows = slice(e * SLOT, (e + 1) * SLOT)
                so[rows, :] = nn(hid[rows, :], wd[e]).astype(BF16)
            if j in TPF:
                ypart[j, :PACK, :] = nn(pmat[...], so[...]).astype(BF16)
                over[j] = rcopy(ypart.at[j, pl.ds(0, PACK)], yrecv.at[j, pl.ds(0, PACK)], r_y.at[j], 1, tp=1 - tp)
            else:
                back[j] = go_back(j, nn(gmat[...], so[...]))

    def first_leg(j):
        if j in TPF:
            with scope(f"fy{j}"):
                over[j].wait_recv()
            r = (ypart[j, :PACK, :].astype(F32) + yrecv[j, :PACK, :].astype(F32)).astype(BF16)
            back[j] = go_back(j, nn(gpack[...], r))
        else:
            with scope(f"fx{j}"):
                settle(crecv.at[j, pl.ds(0, (EP - 1) * PAIR)], r_c.at[j])
            ypart[j, :TOK, :] = nn(tmat[...], crecv[j]).astype(BF16)
            over[j] = rcopy(ypart.at[j, pl.ds(0, TOK)], yrecv.at[j, pl.ds(0, TOK)], r_y.at[j], 1, tp=1 - tp)

    for j in (0, 1, 2, 3, 4):
        first_leg(j)
    with scope("shrecv"):
        resc.wait()
        shc.wait_recv()
    for j in (0, 1, 2, 3, 4):
        cols = slice(j * NC, (j + 1) * NC)
        base = res_v[:, cols].astype(F32) + (sh_part[:, cols].astype(F32) + sh_recv[:, cols].astype(F32))
        with scope(f"last{j}"):
            if j in TPF:
                settle(crecv.at[j, pl.ds(0, (EP - 1) * PAIR)], r_c.at[j])
            else:
                over[j].wait_recv()
        if j in TPF:
            routed = nn(tmat[...], crecv[j])
        else:
            routed = (ypart[j, :TOK, :].astype(F32) + yrecv[j, :TOK, :].astype(F32)).astype(BF16).astype(F32)
        out_ref[:, cols] = (base + gcol[...] * routed).astype(BF16)
    with scope('sendwait'):
        settle(sd.at[pl.ds(0, 4 * TOK)], snd.at[0])
        back_rows = NCH * (EP - 1) * PAIR + len(TPF) * PACK + (NCH - len(TPF)) * TOK
        settle(sd.at[pl.ds(0, back_rows // 2), pl.ds(0, 2 * NC)], snd.at[1])
        settle(ids.at[pl.ds(0, EP - 1)], snd.at[2])


def solution(mesh):
    tok_spec, id_spec = P(("dp", "ep"), None), P(("dp", "ep"))

    def device_step(normed, residual, w_router, ws_gate, ws_up, ws_down, we_gate, we_up, we_down, first_id, alt_id):
        hbm = pl.BlockSpec(memory_space=pl.ANY)
        vm, dma = pltpu.VMEM, pltpu.SemaphoreType.DMA
        weights = [vm((LOCAL, FFE, n), BF16) for _, n in KC for _ in range(2)]
        scratch = [vm((ALL, n), BF16) for _, n in KC]
        scratch += [vm((TOK, D), BF16), vm((EXPERTS, D), F32), vm((EP, 2, 1, TOK), I32)]
        scratch += [vm((D, FFS), BF16), vm((D, FFS), BF16), vm((FFS, D), BF16)] + weights
        scratch += [vm((SLOTS, n), BF16) for _, n in KC]
        scratch += [vm((SLOTS, FFE), F32), vm((LOCAL, FFE, SLOT), F32), vm((SLOTS, FFE), BF16), vm((TOK, FFS), BF16)]
        scratch += [vm((TOK, D), BF16), vm((TOK, D), BF16), vm((EP * PAIR, SLOTS), BF16), vm((TOK, EP * PAIR), BF16), vm((TOK, 1), F32)]
        scratch += [vm((NCH, EP * PAIR, NC), BF16), vm((NCH, EP * PAIR, NC), BF16), vm((NCH, PACK, NC), BF16), vm((NCH, PACK, NC), BF16), vm((2, SLOTS, NC), BF16), vm((GRP - DIRECT, 256, FFE), BF16), vm((GRP - DIRECT, 256, FFE), BF16), vm((EP * PAIR, PACK), BF16), vm((PACK, SLOTS), BF16)]
        scratch += [dma((7,)), dma((len(KC), NGRP // 2)), dma((NCH,)), dma((3,)), dma((1,)), dma((len(KC),)), dma((len(KC),)), dma((1,)), dma((NCH,)), dma((NCH,))]
        return pl.pallas_call(
            kernel,
            out_shape=pltpu.VMEM((TOK, D), BF16),
            in_specs=[hbm] * 11,
            out_specs=pl.BlockSpec(memory_space=pltpu.VMEM),
            scratch_shapes=scratch,
            compiler_params=pltpu.CompilerParams(collective_id=0, has_side_effects=True, vmem_limit_bytes=65_000_000),
            name="moe_layer",
        )(normed, residual, w_router.T, ws_gate, ws_up, ws_down, jnp.swapaxes(we_gate, 1, 2), jnp.swapaxes(we_up, 1, 2), we_down,
          first_id.reshape(1, TOK), alt_id.reshape(1, TOK))

    return jax.shard_map(device_step, mesh=mesh,
                         in_specs=(tok_spec, tok_spec, P(None, None), P(None, "tp"), P(None, "tp"), P("tp", None), P("ep", None, "tp"),
                                   P("ep", None, "tp"), P("ep", "tp", None), id_spec, id_spec),
                         out_specs=tok_spec, check_vma=False)
```

```python
import functools

import jax
import jax.numpy as jnp
from jax import lax
from jax.experimental import pallas as pl
from jax.experimental.pallas import tpu as pltpu
from jax.sharding import PartitionSpec as P

MESH = pl.DeviceIdType.MESH
scope = jax.named_scope
F32, BF16, I32 = jnp.float32, jnp.bfloat16, jnp.int32

EP = 4
TOK = 128
ALL = EP * TOK
EXPERTS = 64
LOCAL = EXPERTS // EP
CAP = 10
SLOT = 16
SLOTS = LOCAL * SLOT
PAIR = 64
D = 1280
FFE = 448
FFS = 896
GRP = 4
NGRP = LOCAL // GRP
DIRECT = 1
KC = tuple((k, 256) for k in range(0, D, 256))
NC = 256
NCH = D // NC
TPF = (1, 3)
PACK = LOCAL * CAP


def nn(a, b):
    return lax.dot_general(a, b, (((1,), (0,)), ((), ())), preferred_element_type=F32)


def nt(a, b):
    return lax.dot_general(a, b, (((1,), (1,)), ((), ())), preferred_element_type=F32)


def silu_mul(g, u):
    return (g * (1.0 / (1.0 + jnp.exp(-g))) * u).astype(BF16)


def kernel(normed, residual, wr, wsg, wsu, wsd, weg, weu, wed, fid, aid, out_ref,
           x0, x1, x2, x3, x4, res_v, wr_v, ids,
           sg, su, sd, w1g, w1u, w2g, w2u, w3g, w3u, w4g, w4u, w5g, w5u,
           xs0, xs1, xs2, xs3, xs4, accg, accu, hid, hid_s,
           sh_part, sh_recv, gmat, tmat, gcol, csend, crecv, ypart, yrecv, slot_out, wt0, wt1, gpack, pmat,
           l_sem, w_sem, d_sem, snd, r_id, r_x, r_core, r_sh, r_c, r_y):
    me = lax.axis_index("ep")
    tp = lax.axis_index("tp")
    xpeer = lax.rem(me + 2, EP)
    cpeer = me + 1 - 2 * lax.rem(me, 2)
    diag = lax.rem(cpeer + 2, EP)
    xr = (x0, x1, x2, x3, x4)
    xsr = (xs0, xs1, xs2, xs3, xs4)
    wgr, wur = (w1g, w2g, w3g, w4g, w5g), (w1u, w2u, w3u, w4u, w5u)
    mine = pl.ds(pl.multiple_of(me * TOK, TOK), TOK)

    def start(c):
        c.start()
        return c

    def settle(ref, sem):
        pltpu.make_async_copy(ref, ref, sem).wait()

    idc = [start(pltpu.make_async_copy(fid, ids.at[me, 0], l_sem.at[5])),
           start(pltpu.make_async_copy(aid, ids.at[me, 1], l_sem.at[5]))]
    xc = [start(pltpu.make_async_copy(normed.at[:, pl.ds(k, n)], xr[c].at[mine], l_sem.at[0])) for c, (k, n) in enumerate(KC)]
    wrc = start(pltpu.make_async_copy(wr, wr_v, l_sem.at[1]))

    def gu_copy(p, h, i):
        k, n = KC[p]
        part = pl.ds(2 * GRP * h, 2 * GRP)
        return pltpu.make_async_copy((weg, weu)[i].at[part, :, pl.ds(k, n)], (wgr, wur)[i][p].at[part], w_sem.at[p, h])

    def d_buf(j):
        return (w1g, w1u, w2g, w2u, w3g)[j]

    def d_copy(j):
        return pltpu.make_async_copy(wed.at[:, :, pl.ds(j * NC, NC)], d_buf(j), d_sem.at[j])

    def start_pass(p):
        for h in range(NGRP // 2):
            for i in range(2):
                gu_copy(p, h, i).start()

    with scope("barrier"):
        bar = pltpu.get_barrier_semaphore()
        for o in (xpeer, cpeer, diag):
            pl.semaphore_signal(bar, inc=1, device_id={"ep": o}, device_id_type=MESH)
        pl.semaphore_signal(bar, inc=1, device_id={"tp": 1 - tp}, device_id_type=MESH)
        settle(ids.at[0], l_sem.at[5])
        settle(sh_recv, l_sem.at[0])
        swc = [start(pltpu.make_async_copy(s, d, l_sem.at[(2, 3, 6)[i]])) for i, (s, d) in enumerate(((wsg, sg), (wsu, su), (wsd, sd)))]
        pl.semaphore_wait(bar, 4)

    sends = []

    def rcopy(src, dst, r, s, **dev):
        c = pltpu.make_async_remote_copy(src_ref=src, dst_ref=dst, send_sem=snd.at[s], recv_sem=r, device_id=dev, device_id_type=MESH)
        c.start()
        sends.append(c)
        return c

    for d in range(1, EP):
        o = lax.rem(me + d, EP)
        rcopy(ids.at[me], ids.at[me], r_id.at[0], 2, ep=o)
    with scope("xsend"):
        xsend, csnd, fwd = [], [], []
        for c in range(len(KC)):
            xsend.append(rcopy(xr[c].at[mine], xr[c].at[mine], r_x.at[c], 0, ep=xpeer))
        for c in range(len(KC)):
            csnd.append(rcopy(xr[c].at[mine], xr[c].at[mine], r_core.at[c], 0, ep=cpeer))

    start_pass(0)
    theirs = pl.ds(pl.multiple_of(xpeer * TOK, TOK), TOK)

    def forward(c):
        with scope(f"fwait{c}"):
            xsend[c].wait_recv()
        fwd.append(rcopy(xr[c].at[theirs], xr[c].at[theirs], r_core.at[c], 0, ep=cpeer))

    xo = [xr[c][mine, :] for c in range(len(KC))]
    with scope("router"):
        wrc.wait()
        wr_hi = wr_v[...].astype(BF16)
        wr_lo = (wr_v[...] - wr_hi.astype(F32)).astype(BF16)
        logits = jnp.zeros((TOK, EXPERTS), F32)
        for c, (k, kn) in enumerate(KC):
            logits = logits + nt(xo[c], wr_hi[:, k:k + kn]) + nt(xo[c], wr_lo[:, k:k + kn])
        ex = jnp.exp(logits - jnp.max(logits, axis=1, keepdims=True))
        prob = ex / jnp.sum(ex, axis=1, keepdims=True)
    with scope("shwait"):
        swc[0].wait()
        swc[1].wait()
    resc = start(pltpu.make_async_copy(residual, res_v, l_sem.at[4]))
    with scope("shgu"):
        for n0 in range(0, FFS, 256):
            n = min(256, FFS - n0)
            g = sum(nn(xr[c][mine, :], sg[k:k + kn, n0:n0 + n]) for c, (k, kn) in enumerate(KC))
            u = sum(nn(xr[c][mine, :], su[k:k + kn, n0:n0 + n]) for c, (k, kn) in enumerate(KC))
            hid_s[:, n0:n0 + n] = silu_mul(g, u)
    with scope("shdown"):
        swc[2].wait()
        for n0 in range(0, D, 256):
            sh_part[:, n0:n0 + 256] = nn(hid_s[...], sd[:, n0:n0 + 256]).astype(BF16)
    start_pass(1)
    start_pass(2)

    forward(0)
    shc = rcopy(sh_part, sh_recv, r_sh.at[0], 0, tp=1 - tp)

    with scope("idwait"):
        settle(ids.at[pl.ds(0, EP - 1)], r_id.at[0])
    with scope("routing"):
        f = jnp.concatenate([ids[o, 0] for o in range(EP)], axis=1)
        a = jnp.concatenate([ids[o, 1] for o in range(EP)], axis=1)
        ti, tj = lax.broadcasted_iota(I32, (ALL, ALL), 0), lax.broadcasted_iota(I32, (ALL, ALL), 1)
        before = jnp.where(ti < tj, 1.0, 0.0)
        before_dev = jnp.where((ti // TOK) == (tj // TOK), before, 0.0).astype(BF16)
        before = before.astype(BF16)
        eio = lax.broadcasted_iota(I32, (EXPERTS, ALL), 0)
        one_f = jnp.where(eio == f, 1.0, 0.0)
        one_a = jnp.where(eio == a, 1.0, 0.0)
        rank_f = jnp.sum(nn(one_f.astype(BF16), before) * one_f, axis=0, keepdims=True)
        kept = rank_f < CAP - 0.5
        load = jnp.minimum(jnp.sum(one_f, axis=1, keepdims=True), float(CAP))
        over_a = one_a * jnp.where(kept, 0.0, 1.0)
        rank_a = jnp.sum(nn(over_a.astype(BF16), before) * over_a, axis=0, keepdims=True)
        load_a = jnp.sum(one_a * load, axis=0, keepdims=True)
        active = kept | (rank_a + load_a < CAP - 0.5)
        chosen = jnp.where(kept, f, a)
        slot = jnp.where(kept, rank_f, load_a + rank_a).astype(I32)
        owner = chosen // LOCAL
        local = chosen - owner * LOCAL
        here = active & (owner == me)
        slot_code = jnp.where(here, local * SLOT + slot, -1)
        oio = lax.broadcasted_iota(I32, (16, ALL), 0)
        own_f = jnp.where(oio == f // LOCAL, 1.0, 0.0)
        own_a = jnp.where(oio == a // LOCAL + EP, 1.0, 0.0)
        seen = nn((own_f + own_a).astype(BF16), before_dev)
        pos_f = jnp.sum(seen * own_f, axis=0, keepdims=True)
        pos_a = jnp.sum(seen * own_a, axis=0, keepdims=True)
        pos = jnp.where(kept, pos_f, pos_a + PAIR // 2).astype(I32)
        origin = lax.broadcasted_iota(I32, (1, ALL), 1) // TOK
        pair_code = jnp.where(here, origin * PAIR + pos, -1)
        back_code = jnp.where(active, owner * PAIR + pos, -1)
        sio = lax.broadcasted_iota(I32, (SLOTS, ALL), 0)
        smat = jnp.where(sio == slot_code, 1.0, 0.0).astype(BF16)
        rmat = jnp.where(sio == pair_code, 1.0, 0.0).astype(BF16)
        gmat[...] = nt(rmat, smat).astype(BF16)
        pio = lax.broadcasted_iota(I32, (PACK, ALL), 0)
        gpack[...] = nt(rmat, jnp.where(pio == jnp.where(here, local * CAP + slot, -1), 1.0, 0.0).astype(BF16)).astype(BF16)
        col = lax.broadcasted_iota(I32, (PACK, SLOTS), 1)
        packed_row = jnp.where(col % SLOT < CAP, (col // SLOT) * CAP + col % SLOT, -1)
        pmat[...] = jnp.where(lax.broadcasted_iota(I32, (PACK, SLOTS), 0) == packed_row, 1.0, 0.0).astype(BF16)

        own_back, own_chosen = back_code[:, :TOK], jnp.where(active, chosen, -1)[:, :TOK]
        all_chosen = jnp.where(active, chosen, -1)
        for o in range(1, EP):
            cols = slice(o * TOK, (o + 1) * TOK)
            own_back = jnp.where(me == o, back_code[:, cols], own_back)
            own_chosen = jnp.where(me == o, all_chosen[:, cols], own_chosen)
        eye = jnp.where(lax.broadcasted_iota(I32, (TOK, TOK), 0) == lax.broadcasted_iota(I32, (TOK, TOK), 1), 1.0, 0.0).astype(BF16)
        bio = lax.broadcasted_iota(I32, (EP * PAIR, TOK), 0)
        tmat[...] = nt(eye, jnp.where(bio == own_back, 1.0, 0.0).astype(BF16)).astype(BF16)
        cio = lax.broadcasted_iota(I32, (EXPERTS, TOK), 0)
        pick = nt(eye, jnp.where(cio == own_chosen, 1.0, 0.0).astype(BF16))
        gcol[...] = jnp.sum(prob * pick, axis=1, keepdims=True)

    def gather(c):
        with scope(f"xwait{c}"):
            settle(xr[c].at[pl.ds(0, 2 * TOK)], r_core.at[c])
        with scope(f"gather{c}"):
            xsr[c][...] = nn(smat, xr[c][...]).astype(BF16)

    steps = [(p, g) for p in range(len(KC)) for g in range(NGRP)]
    wts = (wt0, wt1)

    def arrived(s):
        p, g = steps[s]
        if g % 2 == 0:
            settle(wgr[p], w_sem.at[p, g // 2])

    def turn(s, i):
        p, g = steps[s]
        if i < GRP - DIRECT:
            wts[s % 2][i, :KC[p][1], :] = wgr[p][g * GRP + i].T

    def gu_expert(s, i):
        p, g = steps[s]
        n = KC[p][1]
        e = g * GRP + i
        rows = slice(e * SLOT, (e + 1) * SLOT)
        xe = xsr[p][rows, :]
        dg = nn(xe, wts[s % 2][i, :n, :]) if i < GRP - DIRECT else nt(xe, wgr[p][e])
        if p == 0:
            accg[rows, :] = dg
        elif p < len(KC) - 1:
            accg[rows, :] += dg
        for r in range(0, FFE, FFE // 2):
            half = slice(r, r + FFE // 2)
            du = nt(wur[p][e, half, :], xe)
            if p == 0:
                accu[e, half, :] = du
            else:
                accu[e, half, :] += du
        if p == len(KC) - 1:
            hid[rows, :] = silu_mul(accg[rows, :] + dg, accu[e].T)

    def gu_steps(lo, hi):
        with scope(f"gu{lo}"):
            for s in range(lo, hi):
                if s + 1 < len(steps):
                    arrived(s + 1)
            for s in range(lo, hi):
                for i in range(GRP):
                    if s + 1 < len(steps):
                        turn(s + 1, i)
                    gu_expert(s, i)

    start_pass(3)
    arrived(0)
    for i in range(GRP):
        turn(0, i)
    gather(0)
    for p in range(len(KC)):
        if p > 0:
            gather(p)
        if p + 1 < len(KC):
            forward(p + 1)
        gu_steps(NGRP * p, NGRP * p + 2)
        if p == 1:
            start_pass(4)
        gu_steps(NGRP * p + 2, NGRP * p + 4)
        for j in {2: (0, 1), 3: (2, 3, 4)}.get(p, ()):
            d_copy(j).start()

    my_rows = pl.ds(pl.multiple_of(me * PAIR, PAIR), PAIR)

    def go_back(j, rows):
        csend[j] = rows.astype(BF16)
        crecv[j, my_rows, :] = csend[j, my_rows, :]
        out = []
        for d in range(1, EP):
            o = lax.rem(me + d, EP)
            out.append(rcopy(csend.at[j, pl.ds(pl.multiple_of(o * PAIR, PAIR), PAIR)], crecv.at[j, my_rows], r_c.at[j], 1, ep=o))
        return out

    back, over = {}, {}
    for j in range(NCH):
        with scope(f"dw{j}"):
            d_copy(j).wait()
        with scope(f"dn{j}"):
            so, wd = slot_out.at[j % 2], d_buf(j)
            for e in range(LOCAL):
                rows = slice(e * SLOT, (e + 1) * SLOT)
                so[rows, :] = nn(hid[rows, :], wd[e]).astype(BF16)
            if j in TPF:
                ypart[j, :PACK, :] = nn(pmat[...], so[...]).astype(BF16)
                over[j] = rcopy(ypart.at[j, pl.ds(0, PACK)], yrecv.at[j, pl.ds(0, PACK)], r_y.at[j], 1, tp=1 - tp)
            else:
                back[j] = go_back(j, nn(gmat[...], so[...]))

    def first_leg(j):
        if j in TPF:
            with scope(f"fy{j}"):
                over[j].wait_recv()
            r = (ypart[j, :PACK, :].astype(F32) + yrecv[j, :PACK, :].astype(F32)).astype(BF16)
            back[j] = go_back(j, nn(gpack[...], r))
        else:
            with scope(f"fx{j}"):
                settle(crecv.at[j, pl.ds(0, (EP - 1) * PAIR)], r_c.at[j])
            ypart[j, :TOK, :] = nn(tmat[...], crecv[j]).astype(BF16)
            over[j] = rcopy(ypart.at[j, pl.ds(0, TOK)], yrecv.at[j, pl.ds(0, TOK)], r_y.at[j], 1, tp=1 - tp)

    for j in (0, 1, 2, 3, 4):
        first_leg(j)
    with scope("shrecv"):
        resc.wait()
        shc.wait_recv()
    for j in (0, 1, 2, 3, 4):
        cols = slice(j * NC, (j + 1) * NC)
        base = res_v[:, cols].astype(F32) + (sh_part[:, cols].astype(F32) + sh_recv[:, cols].astype(F32))
        with scope(f"last{j}"):
            if j in TPF:
                settle(crecv.at[j, pl.ds(0, (EP - 1) * PAIR)], r_c.at[j])
            else:
                over[j].wait_recv()
        if j in TPF:
            routed = nn(tmat[...], crecv[j])
        else:
            routed = (ypart[j, :TOK, :].astype(F32) + yrecv[j, :TOK, :].astype(F32)).astype(BF16).astype(F32)
        out_ref[:, cols] = (base + gcol[...] * routed).astype(BF16)
    with scope('sendwait'):
        settle(sd.at[pl.ds(0, 4 * TOK)], snd.at[0])
        back_rows = NCH * (EP - 1) * PAIR + len(TPF) * PACK + (NCH - len(TPF)) * TOK
        settle(sd.at[pl.ds(0, back_rows // 2), pl.ds(0, 2 * NC)], snd.at[1])
        settle(ids.at[pl.ds(0, EP - 1)], snd.at[2])


def solution(mesh):
    tok_spec, id_spec = P(("dp", "ep"), None), P(("dp", "ep"))

    def device_step(normed, residual, w_router, ws_gate, ws_up, ws_down, we_gate, we_up, we_down, first_id, alt_id):
        hbm = pl.BlockSpec(memory_space=pl.ANY)
        vm, dma = pltpu.VMEM, pltpu.SemaphoreType.DMA
        weights = [vm((LOCAL, FFE, n), BF16) for _, n in KC for _ in range(2)]
        scratch = [vm((ALL, n), BF16) for _, n in KC]
        scratch += [vm((TOK, D), BF16), vm((EXPERTS, D), F32), vm((EP, 2, 1, TOK), I32)]
        scratch += [vm((D, FFS), BF16), vm((D, FFS), BF16), vm((FFS, D), BF16)] + weights
        scratch += [vm((SLOTS, n), BF16) for _, n in KC]
        scratch += [vm((SLOTS, FFE), F32), vm((LOCAL, FFE, SLOT), F32), vm((SLOTS, FFE), BF16), vm((TOK, FFS), BF16)]
        scratch += [vm((TOK, D), BF16), vm((TOK, D), BF16), vm((EP * PAIR, SLOTS), BF16), vm((TOK, EP * PAIR), BF16), vm((TOK, 1), F32)]
        scratch += [vm((NCH, EP * PAIR, NC), BF16), vm((NCH, EP * PAIR, NC), BF16), vm((NCH, PACK, NC), BF16), vm((NCH, PACK, NC), BF16), vm((2, SLOTS, NC), BF16), vm((GRP - DIRECT, 256, FFE), BF16), vm((GRP - DIRECT, 256, FFE), BF16), vm((EP * PAIR, PACK), BF16), vm((PACK, SLOTS), BF16)]
        scratch += [dma((7,)), dma((len(KC), NGRP // 2)), dma((NCH,)), dma((3,)), dma((1,)), dma((len(KC),)), dma((len(KC),)), dma((1,)), dma((NCH,)), dma((NCH,))]
        return pl.pallas_call(
            kernel,
            out_shape=pltpu.VMEM((TOK, D), BF16),
            in_specs=[hbm] * 11,
            out_specs=pl.BlockSpec(memory_space=pltpu.VMEM),
            scratch_shapes=scratch,
            compiler_params=pltpu.CompilerParams(collective_id=0, has_side_effects=True, vmem_limit_bytes=65_000_000),
            name="moe_layer",
        )(normed, residual, w_router.T, ws_gate, ws_up, ws_down, jnp.swapaxes(we_gate, 1, 2), jnp.swapaxes(we_up, 1, 2), we_down,
          first_id.reshape(1, TOK), alt_id.reshape(1, TOK))

    return jax.shard_map(device_step, mesh=mesh,
                         in_specs=(tok_spec, tok_spec, P(None, None), P(None, "tp"), P(None, "tp"), P("tp", None), P("ep", None, "tp"),
                                   P("ep", None, "tp"), P("ep", "tp", None), id_spec, id_spec),
                         out_specs=tok_spec, check_vma=False)
```
